8 devices in a mesh: dp: 2 (over z, y), ep: 4 (over x, core).
Axes of the slice: x: 2, y: 2, z: 1, core: 2. Of those that a mesh axis runs over, the one named last changes fastest.
Arguments:
- x_in: bfloat16 [4096, 512], P(('dp', 'ep')), parts along dimension 0
- idx_a: int32 [4096, 2], P(('dp', 'ep')), parts along dimension 0
- idx_b: int32 [4096, 2], P(('dp', 'ep')), parts along dimension 0
- gate_a: float32 [4096, 2], P(('dp', 'ep')), parts along dimension 0
- gate_b: float32 [4096, 2], P(('dp', 'ep')), parts along dimension 0
- dy_out: bfloat16 [4096, 512], P(('dp', 'ep')), parts along dimension 0
- w1_a: bfloat16 [8, 512, 1792], P('ep')
- w3_a: bfloat16 [8, 512, 1792], P('ep')
- w2_a: bfloat16 [8, 1792, 512], P('ep')
- w1_b: bfloat16 [8, 512, 1792], P('ep')
- w3_b: bfloat16 [8, 512, 1792], P('ep')
- w2_b: bfloat16 [8, 1792, 512], P('ep')
Outputs:
- output 1: bfloat16 [4096, 512], P(('dp', 'ep')), parts along dimension 0
- output 2: bfloat16 [4096, 512], P(('dp', 'ep')), parts along dimension 0
- output 3: float32 [16, 512, 1792], P(('dp', 'ep')), parts along dimension 0
- output 4: float32 [16, 512, 1792], P(('dp', 'ep')), parts along dimension 0
- output 5: float32 [16, 1792, 512], P(('dp', 'ep')), parts along dimension 0
- output 6: float32 [16, 512, 1792], P(('dp', 'ep')), parts along dimension 0
- output 7: float32 [16, 512, 1792], P(('dp', 'ep')), parts along dimension 0
- output 8: float32 [16, 1792, 512], P(('dp', 'ep')), parts along dimension 0
- output 9: float32 [4096, 2], P(('dp', 'ep')), parts along dimension 0
- output 10: float32 [4096, 2], P(('dp', 'ep')), parts along dimension 0
There are 2 independent parts. The reference program is written for one: setup_inputs(seed, part) draws one part's arguments, and reference() takes and returns one part's arrays. A program takes and returns all parts, laid end to end along the dimension named above; an argument that names none is the same for every part.
All inputs are finite; a program needn't handle non-finite values.
Results may differ from the reference program's by a relative error of at most 0.00787.
Values are sent between devices in bfloat16 or wider.
A program may use at most 1 GiB of HBM per device.

```python
import jax
import jax.numpy as jnp
from jax import lax

TOKENS = 512
D = 512
FF = 1792
EXPERTS = 8
TOP = 2
GROUP = 4
CAP = 512
HOT = 1


def draw_routing(root_key):
    key_hot, key_dev = jax.random.split(root_key)
    ranking = jax.random.permutation(key_hot, EXPERTS)
    cold_total = EXPERTS - HOT
    spare_pairs = TOKENS * TOP - HOT * CAP
    base_count = spare_pairs // cold_total
    extra_count = spare_pairs - base_count * cold_total

    def one_device(dev_key):
        key_count, key_rows, key_shift = jax.random.split(dev_key, 3)
        cold_rank = jax.random.permutation(key_count, cold_total)
        cold_count = base_count + (cold_rank < extra_count).astype(jnp.int32)
        by_rank = jnp.concatenate([jnp.full((HOT,), CAP, jnp.int32), cold_count])
        expert_count = jnp.zeros((EXPERTS,), jnp.int32).at[ranking].set(by_rank)
        run_ends = jnp.cumsum(expert_count)
        positions = jnp.arange(TOKENS * TOP, dtype=jnp.int32)
        sorted_ids = jnp.searchsorted(run_ends, positions, side="right").astype(jnp.int32)
        id_table = sorted_ids.reshape(TOP, TOKENS).T
        id_table = id_table[jax.random.permutation(key_rows, TOKENS)]
        row_shift = jax.random.randint(key_shift, (TOKENS, 1), 0, TOP)
        col_order = (jnp.arange(TOP)[None, :] + row_shift) % TOP
        return jnp.take_along_axis(id_table, col_order, axis=1)

    return jax.vmap(one_device)(jax.random.split(key_dev, GROUP)).reshape(GROUP * TOKENS, TOP)


def setup_inputs(seed: int = 0, part: int = 0) -> dict:
    root_key = jax.random.key(seed)
    shared_keys = jax.random.split(root_key, 6)
    part_keys = jax.random.split(jax.random.fold_in(root_key, part), 6)
    row_total = GROUP * TOKENS
    gate_scale = 1.5 / TOP ** 0.5
    in_scale = D ** -0.5
    mid_scale = FF ** -0.5
    x_in = jax.random.normal(part_keys[0], (row_total, D), jnp.float32).astype(jnp.bfloat16)
    idx_a = draw_routing(part_keys[1])
    idx_b = draw_routing(part_keys[2])
    gate_a = (0.5 + jax.random.uniform(part_keys[3], (row_total, TOP), jnp.float32)) * gate_scale
    gate_b = (0.5 + jax.random.uniform(part_keys[4], (row_total, TOP), jnp.float32)) * gate_scale
    dy_out = jax.random.normal(part_keys[5], (row_total, D), jnp.float32).astype(jnp.bfloat16)
    w1_a = (jax.random.normal(shared_keys[0], (EXPERTS, D, FF), jnp.float32) * in_scale).astype(jnp.bfloat16)
    w3_a = (jax.random.normal(shared_keys[1], (EXPERTS, D, FF), jnp.float32) * in_scale).astype(jnp.bfloat16)
    w2_a = (jax.random.normal(shared_keys[2], (EXPERTS, FF, D), jnp.float32) * mid_scale).astype(jnp.bfloat16)
    w1_b = (jax.random.normal(shared_keys[3], (EXPERTS, D, FF), jnp.float32) * in_scale).astype(jnp.bfloat16)
    w3_b = (jax.random.normal(shared_keys[4], (EXPERTS, D, FF), jnp.float32) * in_scale).astype(jnp.bfloat16)
    w2_b = (jax.random.normal(shared_keys[5], (EXPERTS, FF, D), jnp.float32) * mid_scale).astype(jnp.bfloat16)
    return {"x_in": x_in, "idx_a": idx_a, "idx_b": idx_b, "gate_a": gate_a, "gate_b": gate_b, "dy_out": dy_out, "w1_a": w1_a, "w3_a": w3_a, "w2_a": w2_a, "w1_b": w1_b, "w3_b": w3_b, "w2_b": w2_b}


def expert_forward(u_rows, w_gate, w_up, w_down):
    pre_gate = jnp.dot(u_rows, w_gate, preferred_element_type=jnp.float32)
    pre_up = jnp.dot(u_rows, w_up, preferred_element_type=jnp.float32)
    hidden = (jax.nn.silu(pre_gate) * pre_up).astype(jnp.bfloat16)
    out_rows = jnp.dot(hidden, w_down, preferred_element_type=jnp.float32).astype(jnp.bfloat16)
    return pre_gate, pre_up, hidden, out_rows


def device_slots(flat_ids):
    onehot = (flat_ids[:, None] == jnp.arange(EXPERTS, dtype=jnp.int32)[None, :]).astype(jnp.int32)
    return jnp.sum(jnp.cumsum(onehot, axis=0) * onehot, axis=1) - 1


def expert_table(ids):
    per_device = ids.reshape(GROUP, TOKENS * TOP)
    pair_slot = lax.map(device_slots, per_device)
    expert_row = jnp.arange(GROUP, dtype=jnp.int32)[:, None] * CAP + pair_slot
    pair_ids = jnp.arange(GROUP * TOKENS * TOP, dtype=jnp.int32).reshape(GROUP, TOKENS * TOP)
    empty_pair = GROUP * TOKENS * TOP
    return jnp.full((EXPERTS, GROUP * CAP), empty_pair, jnp.int32).at[per_device, expert_row].set(pair_ids)


def layer_forward(x_rows, gates, table, w_gate, w_up, w_down):
    x_pad = jnp.concatenate([x_rows, jnp.zeros((1, D), x_rows.dtype)])
    gate_pad = jnp.concatenate([gates.reshape(-1), jnp.zeros((1,), gates.dtype)])

    def expert_step(out_acc, step_in):
        pair_ids, gate_w, up_w, down_w = step_in
        tok_index = pair_ids // TOP
        out_rows = expert_forward(x_pad[tok_index], gate_w, up_w, down_w)[3]
        weighted = gate_pad[pair_ids][:, None] * out_rows.astype(jnp.float32)
        return out_acc.at[tok_index].add(weighted), None

    out_acc = jnp.zeros((GROUP * TOKENS + 1, D), jnp.float32)
    out_acc = lax.scan(expert_step, out_acc, (table, w_gate, w_up, w_down))[0]
    return (x_rows.astype(jnp.float32) + out_acc[:-1]).astype(jnp.bfloat16)


def layer_backward(dy_rows, x_rows, gates, table, w_gate, w_up, w_down):
    x_pad = jnp.concatenate([x_rows, jnp.zeros((1, D), x_rows.dtype)])
    dy_pad = jnp.concatenate([dy_rows, jnp.zeros((1, D), dy_rows.dtype)])
    gate_pad = jnp.concatenate([gates.reshape(-1), jnp.zeros((1,), gates.dtype)])

    def expert_step(carry_in, step_in):
        dx_acc, dgate_acc = carry_in
        pair_ids, gate_w, up_w, down_w = step_in
        tok_index = pair_ids // TOP
        u_rows = x_pad[tok_index]
        dy_exp = dy_pad[tok_index].astype(jnp.float32)
        pre_gate, pre_up, hidden, out_rows = expert_forward(u_rows, gate_w, up_w, down_w)
        dgate_rows = jnp.sum(dy_exp * out_rows.astype(jnp.float32), axis=1)
        d_out = (gate_pad[pair_ids][:, None] * dy_exp).astype(jnp.bfloat16)
        dw_down = jnp.dot(hidden.T, d_out, preferred_element_type=jnp.float32)
        d_hidden = jnp.dot(d_out, down_w.T, preferred_element_type=jnp.float32)
        gate_sig = jax.nn.sigmoid(pre_gate)
        d_pre_gate = (d_hidden * pre_up * gate_sig * (1.0 + pre_gate * (1.0 - gate_sig))).astype(jnp.bfloat16)
        d_pre_up = (d_hidden * jax.nn.silu(pre_gate)).astype(jnp.bfloat16)
        dw_gate = jnp.dot(u_rows.T, d_pre_gate, preferred_element_type=jnp.float32)
        dw_up = jnp.dot(u_rows.T, d_pre_up, preferred_element_type=jnp.float32)
        du_rows = (jnp.dot(d_pre_gate, gate_w.T, preferred_element_type=jnp.float32) + jnp.dot(d_pre_up, up_w.T, preferred_element_type=jnp.float32)).astype(jnp.bfloat16)
        dx_acc = dx_acc.at[tok_index].add(du_rows.astype(jnp.float32))
        dgate_acc = dgate_acc.at[pair_ids].set(dgate_rows)
        return (dx_acc, dgate_acc), (dw_gate, dw_up, dw_down)

    dx_acc = jnp.zeros((GROUP * TOKENS + 1, D), jnp.float32)
    dgate_acc = jnp.zeros((GROUP * TOKENS * TOP + 1,), jnp.float32)
    (dx_acc, dgate_acc), grads = lax.scan(expert_step, (dx_acc, dgate_acc), (table, w_gate, w_up, w_down))
    dx_rows = (dy_rows.astype(jnp.float32) + dx_acc[:-1]).astype(jnp.bfloat16)
    return dx_rows, dgate_acc[:-1].reshape(GROUP * TOKENS, TOP), grads


def reference(x_in, idx_a, idx_b, gate_a, gate_b, dy_out, w1_a, w3_a, w2_a, w1_b, w3_b, w2_b):
    table_a = expert_table(idx_a)
    table_b = expert_table(idx_b)
    x_mid = layer_forward(x_in, gate_a, table_a, w1_a, w3_a, w2_a)
    x_out = layer_forward(x_mid, gate_b, table_b, w1_b, w3_b, w2_b)
    dx_mid, dgate_b, grads_b = layer_backward(dy_out, x_mid, gate_b, table_b, w1_b, w3_b, w2_b)
    dx_in, dgate_a, grads_a = layer_backward(dx_mid, x_in, gate_a, table_a, w1_a, w3_a, w2_a)
    return (x_out, dx_in, grads_a[0], grads_a[1], grads_a[2], grads_b[0], grads_b[1], grads_b[2], dgate_a, dgate_b)
```

```python
import functools

import jax
import jax.numpy as jnp
from jax import lax
from jax.experimental import pallas as pl
from jax.experimental.pallas import tpu as pltpu
from jax.sharding import PartitionSpec as P

ROWS = 256
TOKS = 256
COLS = 256
VMEM = 66_000_000

BF = jnp.bfloat16
F32 = jnp.float32


def mm(a, b):
    return lax.dot_general(a, b, (((1,), (0,)), ((), ())), preferred_element_type=F32)


def mm_nt(a, b):
    return lax.dot_general(a, b, (((1,), (1,)), ((), ())), preferred_element_type=F32)


def mm_tn(a, b):
    return lax.dot_general(a, b, (((0,), (0,)), ((), ())), preferred_element_type=F32)


def pick_rows(slot_row, base):
    want = lax.broadcasted_iota(jnp.int32, (ROWS, TOKS), 0) + base
    return slot_row == want


def pick_toks(slot_col, base):
    want = lax.broadcasted_iota(jnp.int32, (TOKS, ROWS), 1) + base
    return slot_col == want


def for_blocks(starts_ref, e, base, blocks, body):
    def step(b, carry):
        lo = starts_ref[e, b]
        hi = starts_ref[e, b + 1]

        @pl.when((lo < base + ROWS) & (hi > base) & (hi > lo))
        def _():
            body(b)

        return carry

    lax.fori_loop(0, blocks, step, 0)


def forward_kernel(starts_ref, x_ref, slot_row_ref, slot_col_ref, gate_col_ref, w1_ref, w3_ref, w2_ref, y_ref, u_acc, h_ref):
    e = pl.program_id(0)
    blocks = x_ref.shape[0] // TOKS
    width = w1_ref.shape[2]

    @pl.when(e == 0)
    def _():
        y_ref[...] = jnp.zeros_like(y_ref)

    def tile(k, carry):
        base = k * ROWS
        u_acc[...] = jnp.zeros_like(u_acc)

        def take(b):
            toks = pl.ds(pl.multiple_of(b * TOKS, TOKS), TOKS)
            hot = pick_rows(slot_row_ref[0, b], base).astype(F32).astype(BF)
            u_acc[...] += mm(hot, x_ref[toks, :])

        for_blocks(starts_ref, e, base, blocks, take)
        u = u_acc[...].astype(BF)
        for c in range(0, width, COLS):
            cols = slice(c, c + COLS)
            a = mm(u, w1_ref[0, :, cols])
            b = mm(u, w3_ref[0, :, cols])
            h_ref[:, cols] = (a * jax.nn.sigmoid(a) * b).astype(BF)
        o = mm(h_ref[...], w2_ref[0]).astype(BF)

        def give(b):
            toks = pl.ds(pl.multiple_of(b * TOKS, TOKS), TOKS)
            hot = pick_toks(slot_col_ref[0, toks, :], base).astype(F32).astype(BF)
            y_ref[toks, :] += gate_col_ref[0, toks, :] * mm(hot, o)

        for_blocks(starts_ref, e, base, blocks, give)
        return carry

    count = starts_ref[e, blocks]
    lax.fori_loop(0, (count + ROWS - 1) // ROWS, tile, 0)


def backward_kernel(starts_ref, x_ref, dy_ref, slot_row_ref, slot_col_ref, gate_row_ref, w1_ref, w3_ref, w2_ref,
                    dx_ref, dg_ref, dw1_ref, dw3_ref, dw2_ref, u_acc, dy_acc, g_acc, h_ref, da_ref, db_ref):
    e = pl.program_id(0)
    blocks = x_ref.shape[0] // TOKS
    width = w1_ref.shape[2]

    @pl.when(e == 0)
    def _():
        dx_ref[...] = jnp.zeros_like(dx_ref)

    dg_ref[...] = jnp.zeros_like(dg_ref)
    dw1_ref[...] = jnp.zeros_like(dw1_ref)
    dw3_ref[...] = jnp.zeros_like(dw3_ref)
    dw2_ref[...] = jnp.zeros_like(dw2_ref)

    def tile(k, carry):
        base = k * ROWS
        u_acc[...] = jnp.zeros_like(u_acc)
        dy_acc[...] = jnp.zeros_like(dy_acc)
        g_acc[...] = jnp.zeros_like(g_acc)

        def take(b):
            toks = pl.ds(pl.multiple_of(b * TOKS, TOKS), TOKS)
            pick = pick_rows(slot_row_ref[0, b], base)
            hot = pick.astype(F32).astype(BF)
            u_acc[...] += mm(hot, x_ref[toks, :])
            dy_acc[...] += mm(hot, dy_ref[toks, :])
            g_acc[...] += jnp.sum(jnp.where(pick, gate_row_ref[0, b], 0.0), axis=1, keepdims=True)

        for_blocks(starts_ref, e, base, blocks, take)
        u = u_acc[...].astype(BF)
        q = (g_acc[...] * dy_acc[...]).astype(BF)
        for c in range(0, width, COLS):
            cols = slice(c, c + COLS)
            a = mm(u, w1_ref[0, :, cols])
            b = mm(u, w3_ref[0, :, cols])
            dh = mm_nt(q, w2_ref[0, cols, :])
            s = jax.nn.sigmoid(a)
            act = a * s
            h_ref[:, cols] = (act * b).astype(BF)
            da_ref[:, cols] = (dh * b * s * (1.0 + a * (1.0 - s))).astype(BF)
            db_ref[:, cols] = (dh * act).astype(BF)
        o = mm(h_ref[...], w2_ref[0]).astype(BF)
        dgate = jnp.sum(dy_acc[...] * o.astype(F32), axis=1, keepdims=True)
        for c in range(0, width, COLS):
            cols = slice(c, c + COLS)
            dw2_ref[0, cols, :] += mm_tn(h_ref[:, cols], q)
            dw1_ref[0, :, cols] += mm_tn(u, da_ref[:, cols])
            dw3_ref[0, :, cols] += mm_tn(u, db_ref[:, cols])
        du = (mm_nt(da_ref[...], w1_ref[0]) + mm_nt(db_ref[...], w3_ref[0])).astype(BF)

        def give(b):
            toks = pl.ds(pl.multiple_of(b * TOKS, TOKS), TOKS)
            hot = pick_toks(slot_col_ref[0, toks, :], base).astype(F32).astype(BF)
            dx_ref[toks, :] += mm(hot, du)
            pick = pick_rows(slot_row_ref[0, b], base)
            dg_ref[0, b] += jnp.sum(jnp.where(pick, dgate, 0.0), axis=0, keepdims=True)

        for_blocks(starts_ref, e, base, blocks, give)
        return carry

    count = starts_ref[e, blocks]
    lax.fori_loop(0, (count + ROWS - 1) // ROWS, tile, 0)


def whole(shape):
    return pl.BlockSpec(shape, lambda e, *_: (0,) * len(shape), pipeline_mode=pl.Buffered(1))


def per_expert(shape):
    return pl.BlockSpec((1,) + shape, lambda e, *_: (e,) + (0,) * len(shape))


def run_forward(x, maps, w1, w3, w2):
    tokens, dim = x.shape
    experts, _, width = w1.shape
    blocks = tokens // TOKS
    return pl.pallas_call(
        forward_kernel,
        grid_spec=pltpu.PrefetchScalarGridSpec(
            num_scalar_prefetch=1,
            grid=(experts,),
            in_specs=[
                whole((tokens, dim)),
                per_expert((blocks, 1, TOKS)),
                per_expert((tokens, 1)),
                per_expert((tokens, 1)),
                per_expert((dim, width)),
                per_expert((dim, width)),
                per_expert((width, dim)),
            ],
            out_specs=whole((tokens, dim)),
            scratch_shapes=[pltpu.VMEM((ROWS, dim), F32), pltpu.VMEM((ROWS, width), BF)],
        ),
        out_shape=jax.ShapeDtypeStruct((tokens, dim), F32),
        compiler_params=pltpu.CompilerParams(vmem_limit_bytes=VMEM),
        cost_estimate=pl.CostEstimate(flops=6 * tokens * dim * width, bytes_accessed=6 * experts * dim * width, transcendentals=0),
        name="expert_forward",
    )(maps["starts"], x, maps["slot_row"], maps["slot_col"], maps["gate_col"], w1, w3, w2)


def run_backward(x, dy, maps, w1, w3, w2):
    tokens, dim = x.shape
    experts, _, width = w1.shape
    blocks = tokens // TOKS
    return pl.pallas_call(
        backward_kernel,
        grid_spec=pltpu.PrefetchScalarGridSpec(
            num_scalar_prefetch=1,
            grid=(experts,),
            in_specs=[
                whole((tokens, dim)),
                whole((tokens, dim)),
                per_expert((blocks, 1, TOKS)),
                per_expert((tokens, 1)),
                per_expert((blocks, 1, TOKS)),
                per_expert((dim, width)),
                per_expert((dim, width)),
                per_expert((width, dim)),
            ],
            out_specs=[
                whole((tokens, dim)),
                per_expert((blocks, 1, TOKS)),
                pl.BlockSpec((1, dim, width), lambda e, *_: (e, 0, 0), pipeline_mode=pl.Buffered(1)),
                pl.BlockSpec((1, dim, width), lambda e, *_: (e, 0, 0), pipeline_mode=pl.Buffered(1)),
                pl.BlockSpec((1, width, dim), lambda e, *_: (e, 0, 0), pipeline_mode=pl.Buffered(1)),
            ],
            scratch_shapes=[
                pltpu.VMEM((ROWS, dim), F32),
                pltpu.VMEM((ROWS, dim), F32),
                pltpu.VMEM((ROWS, 1), F32),
                pltpu.VMEM((ROWS, width), BF),
                pltpu.VMEM((ROWS, width), BF),
                pltpu.VMEM((ROWS, width), BF),
            ],
        ),
        out_shape=[
            jax.ShapeDtypeStruct((tokens, dim), F32),
            jax.ShapeDtypeStruct((experts, blocks, 1, TOKS), F32),
            jax.ShapeDtypeStruct((experts, dim, width), F32),
            jax.ShapeDtypeStruct((experts, dim, width), F32),
            jax.ShapeDtypeStruct((experts, width, dim), F32),
        ],
        compiler_params=pltpu.CompilerParams(vmem_limit_bytes=VMEM),
        cost_estimate=pl.CostEstimate(flops=18 * tokens * dim * width, bytes_accessed=18 * experts * dim * width, transcendentals=0),
        name="expert_backward",
    )(maps["starts"], x, dy, maps["slot_row"], maps["slot_col"], maps["gate_row"], w1, w3, w2)


def routing(ids, gates, first, experts):
    tokens = ids.shape[0]
    blocks = tokens // TOKS
    hits = ids.T[None, :, :] == (first + jnp.arange(experts, dtype=jnp.int32))[:, None, None]
    mask = jnp.any(hits, axis=1)
    gate = jnp.sum(jnp.where(hits, gates.T[None], 0.0), axis=1)
    seen = jnp.cumsum(mask.astype(jnp.int32), axis=1)
    slot = jnp.where(mask, seen - 1, -1)
    starts = jnp.concatenate([jnp.zeros((experts, 1), jnp.int32), seen[:, TOKS - 1 :: TOKS]], axis=1)
    return {
        "hits": hits,
        "starts": starts,
        "slot_row": slot.reshape(experts, blocks, 1, TOKS),
        "slot_col": slot[:, :, None],
        "gate_row": gate.reshape(experts, blocks, 1, TOKS),
        "gate_col": gate[:, :, None],
    }


def solution(mesh):
    tok_spec = P(("dp", "ep"))
    w_spec = P("ep")

    def device_program(x_in, idx_a, idx_b, gate_a, gate_b, dy_out, w1_a, w3_a, w2_a, w1_b, w3_b, w2_b):
        experts = w1_a.shape[0]
        first = lax.axis_index("ep").astype(jnp.int32) * experts
        gather = functools.partial(lax.all_gather, axis_name="ep", tiled=True)
        scatter = functools.partial(lax.psum_scatter, axis_name="ep", tiled=True)

        ids = gather(jnp.concatenate([idx_a, idx_b], axis=1))
        gates = gather(jnp.concatenate([gate_a, gate_b], axis=1))
        maps_a = routing(ids[:, :2], gates[:, :2], first, experts)
        maps_b = routing(ids[:, 2:], gates[:, 2:], first, experts)

        def forward(x_own, x_all, maps, w1, w3, w2):
            part = run_forward(x_all, maps, w1, w3, w2)
            return (x_own.astype(F32) + scatter(part)).astype(BF)

        def backward(dy_own, dy_all, x_all, maps, w1, w3, w2):
            part, dg, dw1, dw3, dw2 = run_backward(x_all, dy_all, maps, w1, w3, w2)
            dx = (dy_own.astype(F32) + scatter(part)).astype(BF)
            dg = dg.reshape(experts, 1, -1)
            dgate = scatter(jnp.sum(jnp.where(maps["hits"], dg, 0.0), axis=0).T)
            return dx, dgate, (dw1, dw3, dw2)

        x_all = gather(x_in)
        x_mid = forward(x_in, x_all, maps_a, w1_a, w3_a, w2_a)
        mid_all = gather(x_mid)
        dy_all = gather(dy_out)
        x_out = forward(x_mid, mid_all, maps_b, w1_b, w3_b, w2_b)
        dx_mid, dgate_b, grads_b = backward(dy_out, dy_all, mid_all, maps_b, w1_b, w3_b, w2_b)
        x_again, dx_mid_again = lax.optimization_barrier((x_in, dx_mid))
        dx_in, dgate_a, grads_a = backward(dx_mid, gather(dx_mid_again), gather(x_again), maps_a, w1_a, w3_a, w2_a)
        return (x_out, dx_in) + grads_a + grads_b + (dgate_a, dgate_b)

    return jax.shard_map(device_program, mesh=mesh, in_specs=(tok_spec,) * 6 + (w_spec,) * 6, out_specs=(tok_spec,) * 10, check_vma=False)
```

```python
import jax
import jax.numpy as jnp
from jax import lax
from jax.experimental import pallas as pl
from jax.experimental.pallas import tpu as pltpu
from jax.sharding import PartitionSpec as P

ROWS = 256
TOKS = 256
SPAN = TOKS + 16
COLS = 256
VMEM = 66_000_000

BF = jnp.bfloat16
F32 = jnp.float32


def mm(a, b):
    return lax.dot_general(a, b, (((1,), (0,)), ((), ())), preferred_element_type=F32)


def mm_nt(a, b):
    return lax.dot_general(a, b, (((1,), (1,)), ((), ())), preferred_element_type=F32)


def mm_tn(a, b):
    return lax.dot_general(a, b, (((0,), (0,)), ((), ())), preferred_element_type=F32)


def block_base(starts_ref, e, b):
    return pl.multiple_of((starts_ref[e, b] // 16) * 16, 16)


def tile_count(starts_ref, e, blocks):
    return (starts_ref[e, blocks] + ROWS - 1) // ROWS


def block_of(refs, b):
    per = refs[0].shape[0] // TOKS
    return refs[b // per], slice((b % per) * TOKS, (b % per + 1) * TOKS)


def compact(starts_ref, slot_row_ref, e, blocks, makers, outs):
    for b in range(blocks):
        base = block_base(starts_ref, e, b)
        want = lax.broadcasted_iota(jnp.int32, (SPAN, TOKS), 0) + base
        hot = (slot_row_ref[0, b] == want).astype(F32).astype(BF)
        for make, out in zip(makers, outs):
            rows = mm(hot, make(b)).astype(BF)
            if b == 0:
                out[pl.ds(base, SPAN), :] = rows
            else:
                out[pl.ds(base, 16), :] += rows[:16]
                out[pl.ds(base + 16, TOKS), :] = rows[16:]
    end = block_base(starts_ref, e, blocks - 1) + SPAN
    for out in outs:
        out[pl.ds(end, ROWS), :] = jnp.zeros((ROWS, out.shape[1]), BF)


def spread_hot(starts_ref, slot_col_ref, e, b):
    base = block_base(starts_ref, e, b)
    want = lax.broadcasted_iota(jnp.int32, (TOKS, SPAN), 1) + base
    hot = (slot_col_ref[0, b * TOKS : (b + 1) * TOKS, :] == want).astype(F32).astype(BF)
    return hot, pl.ds(base, SPAN)


def zero_after(starts_ref, e, blocks, ref):
    end = pl.multiple_of(tile_count(starts_ref, e, blocks) * ROWS, ROWS)
    ref[pl.ds(end, SPAN), :] = jnp.zeros((SPAN, ref.shape[1]), BF)


def forward_kernel(starts_ref, x0, x1, x2, x3, slot_row_ref, slot_col_ref, gate_col_ref, w1_ref, w3_ref, w2_ref,
                   y0, y1, y2, y3, u_all, o_all, h_ref):
    e = pl.program_id(0)
    xs, ys = (x0, x1, x2, x3), (y0, y1, y2, y3)
    blocks = slot_row_ref.shape[1]
    width = w1_ref.shape[2]

    def tokens_of(b):
        ref, toks = block_of(xs, b)
        return ref[toks, :]

    compact(starts_ref, slot_row_ref, e, blocks, (tokens_of,), (u_all,))

    def tile(k, carry):
        rows = pl.ds(pl.multiple_of(k * ROWS, ROWS), ROWS)
        u = u_all[rows, :]
        for c in range(0, width, COLS):
            cols = slice(c, c + COLS)
            a = mm(u, w1_ref[0, :, cols])
            b = mm(u, w3_ref[0, :, cols])
            h_ref[:, cols] = (a * jax.nn.sigmoid(a) * b).astype(BF)
        o_all[rows, :] = mm(h_ref[...], w2_ref[0]).astype(BF)
        return carry

    lax.fori_loop(0, tile_count(starts_ref, e, blocks), tile, 0)
    zero_after(starts_ref, e, blocks, o_all)

    def put(add):
        for b in range(blocks):
            hot, rows = spread_hot(starts_ref, slot_col_ref, e, b)
            part = gate_col_ref[0, b * TOKS : (b + 1) * TOKS, :] * mm(hot, o_all[rows, :])
            ref, toks = block_of(ys, b)
            ref[toks, :] = ref[toks, :] + part if add else part

    pl.when(e == 0)(lambda: put(False))
    pl.when(e != 0)(lambda: put(True))


def dx_kernel(starts_ref, x0, x1, x2, x3, g0, g1, g2, g3, slot_row_ref, slot_col_ref, gate_col_ref, w1_ref, w3_ref, w2_ref,
              dx0, dx1, dx2, dx3, rows_hbm, u_all, q_all, du_all, kept, sems):
    e = pl.program_id(0)
    xs, gs, dxs = (x0, x1, x2, x3), (g0, g1, g2, g3), (dx0, dx1, dx2, dx3)
    blocks = slot_row_ref.shape[1]
    dim, width = w1_ref.shape[1:]
    count = tile_count(starts_ref, e, blocks)

    def tokens_of(b):
        ref, toks = block_of(xs, b)
        return ref[toks, :]

    def scaled_of(b):
        ref, toks = block_of(gs, b)
        return (gate_col_ref[0, b * TOKS : (b + 1) * TOKS, :] * ref[toks, :].astype(F32)).astype(BF)

    compact(starts_ref, slot_row_ref, e, blocks, (tokens_of, scaled_of), (u_all, q_all))

    def copy_out(k):
        slot = lax.rem(k, 2)
        rows = pl.ds(pl.multiple_of(k * ROWS, ROWS), ROWS)
        return pltpu.make_async_copy(kept.at[slot], rows_hbm.at[e, rows, :], sems.at[slot])

    def tile(k, carry):
        slot = lax.rem(k, 2)
        rows = pl.ds(pl.multiple_of(k * ROWS, ROWS), ROWS)

        @pl.when(k >= 2)
        def _():
            copy_out(k - 2).wait()

        u = u_all[rows, :]
        q = q_all[rows, :]
        for c in range(0, width, COLS):
            cols = slice(c, c + COLS)
            a = mm(u, w1_ref[0, :, cols])
            b = mm(u, w3_ref[0, :, cols])
            dh = mm_nt(q, w2_ref[0, cols, :])
            s = jax.nn.sigmoid(a)
            act = a * s
            kept[slot, :, c : c + COLS] = (act * b).astype(BF)
            kept[slot, :, width + c : width + c + COLS] = (dh * b * s * (1.0 + a * (1.0 - s))).astype(BF)
            kept[slot, :, 2 * width + c : 2 * width + c + COLS] = (dh * act).astype(BF)
        kept[slot, :, 3 * width : 3 * width + dim] = u
        kept[slot, :, 3 * width + dim :] = q
        du = mm_nt(kept[slot, :, width : 2 * width], w1_ref[0]) + mm_nt(kept[slot, :, 2 * width : 3 * width], w3_ref[0])
        du_all[rows, :] = du.astype(BF)
        copy_out(k).start()
        return carry

    lax.fori_loop(0, count, tile, 0)
    zero_after(starts_ref, e, blocks, du_all)

    def put(add):
        for b in range(blocks):
            hot, rows = spread_hot(starts_ref, slot_col_ref, e, b)
            part = mm(hot, du_all[rows, :])
            ref, toks = block_of(dxs, b)
            ref[toks, :] = ref[toks, :] + part if add else part

    pl.when(e == 0)(lambda: put(False))
    pl.when(e != 0)(lambda: put(True))

    @pl.when(count >= 2)
    def _():
        copy_out(count - 2).wait()

    @pl.when(count >= 1)
    def _():
        copy_out(count - 1).wait()


def dw_kernel(starts_ref, g0, g1, g2, g3, slot_col_ref, rows_hbm, w2_ref, dg_ref, dw1_ref, dw3_ref, dw2_ref, o_all, kept, sems):
    e = pl.program_id(0)
    gs = (g0, g1, g2, g3)
    blocks = slot_col_ref.shape[1] // TOKS
    width, dim = w2_ref.shape[1:]
    count = tile_count(starts_ref, e, blocks)

    def copy_in(k):
        slot = lax.rem(k, 2)
        rows = pl.ds(pl.multiple_of(k * ROWS, ROWS), ROWS)
        return pltpu.make_async_copy(rows_hbm.at[e, rows, :], kept.at[slot], sems.at[slot])

    @pl.when(count >= 1)
    def _():
        copy_in(0).start()

    dw1_ref[...] = jnp.zeros_like(dw1_ref)
    dw3_ref[...] = jnp.zeros_like(dw3_ref)
    dw2_ref[...] = jnp.zeros_like(dw2_ref)

    def tile(k, carry):
        slot = lax.rem(k, 2)
        rows = pl.ds(pl.multiple_of(k * ROWS, ROWS), ROWS)
        copy_in(k).wait()

        @pl.when(k + 1 < count)
        def _():
            copy_in(k + 1).start()

        u = kept[slot, :, 3 * width : 3 * width + dim]
        q = kept[slot, :, 3 * width + dim :]
        for c in range(0, width, COLS):
            cols = slice(c, c + COLS)
            dw2_ref[0, cols, :] += mm_tn(kept[slot, :, c : c + COLS], q)
            dw1_ref[0, :, cols] += mm_tn(u, kept[slot, :, width + c : width + c + COLS])
            dw3_ref[0, :, cols] += mm_tn(u, kept[slot, :, 2 * width + c : 2 * width + c + COLS])
        o_all[rows, :] = mm(kept[slot, :, :width], w2_ref[0]).astype(BF)
        return carry

    lax.fori_loop(0, count, tile, 0)
    zero_after(starts_ref, e, blocks, o_all)
    for b in range(blocks):
        hot, rows = spread_hot(starts_ref, slot_col_ref, e, b)
        o = mm(hot, o_all[rows, :])
        ref, toks = block_of(gs, b)
        dg_ref[0, b * TOKS : (b + 1) * TOKS, :] = jnp.sum(ref[toks, :].astype(F32) * o, axis=1, keepdims=True)


def whole(shape):
    return pl.BlockSpec(shape, lambda e, *_: (0,) * len(shape), pipeline_mode=pl.Buffered(1))


def per_expert(shape):
    return pl.BlockSpec((1,) + shape, lambda e, *_: (e,) + (0,) * len(shape))


def call(kernel, name, experts, maps, operands, in_specs, outs, out_specs, scratch, flops):
    return pl.pallas_call(
        kernel,
        grid_spec=pltpu.PrefetchScalarGridSpec(
            num_scalar_prefetch=1, grid=(experts,), in_specs=in_specs, out_specs=out_specs, scratch_shapes=scratch
        ),
        out_shape=outs,
        compiler_params=pltpu.CompilerParams(vmem_limit_bytes=VMEM),
        cost_estimate=pl.CostEstimate(flops=flops, bytes_accessed=40_000_000, transcendentals=0),
        name=name,
    )(maps["starts"], *operands)


def run_forward(xs, maps, w1, w3, w2):
    tok, dim = xs[0].shape
    tokens = tok * len(xs)
    experts, _, width = w1.shape
    blocks = tokens // TOKS
    most = tokens + SPAN + ROWS
    return call(
        forward_kernel,
        "expert_forward",
        experts,
        maps,
        (*xs, maps["slot_row"], maps["slot_col"], maps["gate_col"], w1, w3, w2),
        [whole((tok, dim))] * 4
        + [per_expert((blocks, 1, TOKS)), per_expert((tokens, 1)), per_expert((tokens, 1))]
        + [per_expert((dim, width)), per_expert((dim, width)), per_expert((width, dim))],
        [jax.ShapeDtypeStruct((tok, dim), F32)] * 4,
        [whole((tok, dim))] * 4,
        [pltpu.VMEM((most, dim), BF), pltpu.VMEM((most, dim), BF), pltpu.VMEM((ROWS, width), BF)],
        2 * 3 * tokens * dim * width,
    )


def run_dx(xs, gs, maps, w1, w3, w2):
    tok, dim = xs[0].shape
    tokens = tok * len(xs)
    experts, _, width = w1.shape
    blocks = tokens // TOKS
    most = tokens + SPAN + ROWS
    kept = 3 * width + 2 * dim
    out = call(
        dx_kernel,
        "expert_dx",
        experts,
        maps,
        (*xs, *gs, maps["slot_row"], maps["slot_col"], maps["gate_col"], w1, w3, w2),
        [whole((tok, dim))] * 8
        + [per_expert((blocks, 1, TOKS)), per_expert((tokens, 1)), per_expert((tokens, 1))]
        + [per_expert((dim, width)), per_expert((dim, width)), per_expert((width, dim))],
        [jax.ShapeDtypeStruct((tok, dim), F32)] * 4 + [jax.ShapeDtypeStruct((experts, tokens, kept), BF)],
        [whole((tok, dim))] * 4 + [pl.BlockSpec(memory_space=pl.ANY)],
        [pltpu.VMEM((most, dim), BF)] * 3 + [pltpu.VMEM((2, ROWS, kept), BF), pltpu.SemaphoreType.DMA((2,))],
        2 * 5 * tokens * dim * width,
    )
    return out[:4], out[4]


def run_dw(gs, rows, maps, w2):
    tok, dim = gs[0].shape
    tokens = tok * len(gs)
    experts, width, _ = w2.shape
    most = tokens + SPAN + ROWS
    kept = rows.shape[2]
    return call(
        dw_kernel,
        "expert_dw",
        experts,
        maps,
        (*gs, maps["slot_col"], rows, w2),
        [whole((tok, dim))] * 4 + [per_expert((tokens, 1)), pl.BlockSpec(memory_space=pl.ANY), per_expert((width, dim))],
        [
            jax.ShapeDtypeStruct((experts, tokens, 1), F32),
            jax.ShapeDtypeStruct((experts, dim, width), F32),
            jax.ShapeDtypeStruct((experts, dim, width), F32),
            jax.ShapeDtypeStruct((experts, width, dim), F32),
        ],
        [per_expert((tokens, 1)), per_expert((dim, width)), per_expert((dim, width)), per_expert((width, dim))],
        [pltpu.VMEM((most, dim), BF), pltpu.VMEM((2, ROWS, kept), BF), pltpu.SemaphoreType.DMA((2,))],
        2 * 4 * tokens * dim * width,
    )


def routing(ids, gates, first, experts):
    tokens = ids.shape[1]
    blocks = tokens // TOKS
    hits = ids[None] == (first + jnp.arange(experts, dtype=F32))[:, None, None]
    mask = jnp.any(hits, axis=1)
    gate = jnp.sum(jnp.where(hits, gates[None], 0.0), axis=1)
    seen = jnp.cumsum(mask.astype(jnp.int32), axis=1)
    slot = jnp.where(mask, seen - 1, -1)
    starts = jnp.concatenate([jnp.zeros((experts, 1), jnp.int32), seen[:, TOKS - 1 :: TOKS]], axis=1)
    return {
        "hits": hits,
        "starts": starts,
        "slot_row": slot.reshape(experts, blocks, 1, TOKS),
        "slot_col": slot[:, :, None],
        "gate_col": gate[:, :, None],
    }


def solution(mesh):
    tok_spec = P(("dp", "ep"))
    w_spec = P("ep")
    across = [(0, 2), (2, 0), (1, 3), (3, 1)]
    beside = [(0, 1), (1, 0), (2, 3), (3, 2)]

    def far(v):
        return lax.ppermute(v, "ep", across)

    def near(v):
        return lax.ppermute(v, "ep", beside)

    def gather(own):
        other = far(own)
        return other, near(other), own, near(own)

    def combine(parts):
        other, diagonal, own, mate = parts
        sent = other + near(diagonal)
        return own + near(mate) + far(sent)

    def device_program(x_in, idx_a, idx_b, gate_a, gate_b, dy_out, w1_a, w3_a, w2_a, w1_b, w3_b, w2_b):
        experts = w1_a.shape[0]
        tok = x_in.shape[0]
        first = (lax.axis_index("ep") * experts).astype(F32)
        own_map = jnp.concatenate([idx_a.astype(F32), idx_b.astype(F32), gate_a, gate_b], axis=1).T
        table = jnp.concatenate(gather(own_map), axis=1)
        maps_a = routing(table[0:2], table[4:6], first, experts)
        maps_b = routing(table[2:4], table[6:8], first, experts)

        def add(base, parts):
            return (base.astype(F32) + combine(parts)).astype(BF)

        def dgate_of(dg, maps):
            part = jnp.sum(jnp.where(maps["hits"], dg.reshape(experts, 1, -1), 0.0), axis=0)
            return combine([part[:, i * tok : (i + 1) * tok] for i in range(4)]).T

        x_all = gather(x_in)
        x_mid = add(x_in, run_forward(x_all, maps_a, w1_a, w3_a, w2_a))
        mid_all = gather(x_mid)
        dy_all = gather(dy_out)
        dx_parts, rows_b = run_dx(mid_all, dy_all, maps_b, w1_b, w3_b, w2_b)
        dx_mid = add(dy_out, dx_parts)
        dg_b, dw1_b, dw3_b, dw2_b = run_dw(dy_all, rows_b, maps_b, w2_b)
        x_out = add(x_mid, run_forward(mid_all, maps_b, w1_b, w3_b, w2_b))
        x_again, _ = lax.optimization_barrier((x_in, x_mid))
        again_all = gather(x_again)
        dmid_all = gather(dx_mid)
        dx_parts, rows_a = run_dx(again_all, dmid_all, maps_a, w1_a, w3_a, w2_a)
        dx_in = add(dx_mid, dx_parts)
        dg_a, dw1_a, dw3_a, dw2_a = run_dw(dmid_all, rows_a, maps_a, w2_a)
        return (x_out, dx_in, dw1_a, dw3_a, dw2_a, dw1_b, dw3_b, dw2_b, dgate_of(dg_a, maps_a), dgate_of(dg_b, maps_b))

    return jax.shard_map(device_program, mesh=mesh, in_specs=(tok_spec,) * 6 + (w_spec,) * 6, out_specs=(tok_spec,) * 10, check_vma=False)
```

```python
import jax
import jax.numpy as jnp
from jax import lax
from jax.experimental import pallas as pl
from jax.experimental.pallas import tpu as pltpu
from jax.sharding import PartitionSpec as P


ROWS = 256
TOKS = 256
SPAN = TOKS + 16
COLS = 256
EXPERTS = 2
VMEM = 66_000_000

BF = jnp.bfloat16
F32 = jnp.float32


def mm(a, b):
    return lax.dot_general(a, b, (((1,), (0,)), ((), ())), preferred_element_type=F32)


def mm_nt(a, b):
    return lax.dot_general(a, b, (((1,), (1,)), ((), ())), preferred_element_type=F32)


def mm_tn(a, b):
    return lax.dot_general(a, b, (((0,), (0,)), ((), ())), preferred_element_type=F32)


def block_of(refs, b):
    per = refs[0].shape[0] // TOKS
    return refs[b // per], slice((b % per) * TOKS, (b % per + 1) * TOKS)


def tile_rows(k):
    return pl.ds(pl.multiple_of(k * ROWS, ROWS), ROWS)


class Slots:
    def __init__(self, layer, starts_ref, rows_ref, cols_ref, blocks):
        self.line = layer * EXPERTS
        self.starts_ref, self.rows_ref, self.cols_ref, self.blocks = starts_ref, rows_ref, cols_ref, blocks

    def tiles(self, e):
        return (self.starts_ref[self.line + e, self.blocks] + ROWS - 1) // ROWS

    def base(self, e, b):
        return pl.multiple_of((self.starts_ref[self.line + e, b] // 16) * 16, 16)

    def col(self, b, i):
        return self.cols_ref[b * TOKS : (b + 1) * TOKS, i : i + 1]

    def gate(self, e, b):
        return self.col(b, EXPERTS + e)

    def choice(self, e, b):
        return self.col(b, 2 * EXPERTS + e)

    def compact(self, e, makers, outs):
        line = lax.broadcasted_iota(jnp.int32, (SPAN, TOKS), 0).astype(F32)
        for b in range(self.blocks):
            base = self.base(e, b)
            slot = self.rows_ref[self.line + e : self.line + e + 1, b * TOKS : (b + 1) * TOKS] - base.astype(F32)
            hot = jnp.where(slot == line, 1.0, 0.0).astype(BF)
            for make, out in zip(makers, outs):
                rows = mm(hot, make(b)).astype(BF)
                if b == 0:
                    out[pl.ds(base, SPAN), :] = rows
                else:
                    out[pl.ds(base, 16), :] += rows[:16]
                    out[pl.ds(base + 16, TOKS), :] = rows[16:]
        end = self.base(e, self.blocks - 1) + SPAN
        for out in outs:
            out[pl.ds(end, ROWS), :] = jnp.zeros((ROWS, out.shape[1]), BF)

    def spread(self, e, b, ref):
        base = self.base(e, b)
        line = lax.broadcasted_iota(jnp.int32, (TOKS, SPAN), 1).astype(F32)
        hot = jnp.where(self.col(b, e) - base.astype(F32) == line, 1.0, 0.0).astype(BF)
        return mm(hot, ref[pl.ds(base, SPAN), :])

    def zero_after(self, e, ref):
        end = pl.multiple_of(self.tiles(e) * ROWS, ROWS)
        ref[pl.ds(end, SPAN), :] = jnp.zeros((SPAN, ref.shape[1]), BF)


def routing_kernel(t0, t1, t2, t3, rows_ref, cols_a_ref, cols_b_ref, starts_ref):
    tables = (t0, t1, t2, t3)
    tok = t0.shape[1]
    blocks = len(tables) * tok // TOKS
    first = (lax.axis_index("ep") * EXPERTS).astype(F32)
    line = lax.broadcasted_iota(jnp.int32, (8, TOKS), 0)
    target = first + (line % EXPERTS).astype(F32)
    lane = lax.broadcasted_iota(jnp.int32, (8, 128), 1)
    upto = (lax.broadcasted_iota(jnp.int32, (TOKS, TOKS), 0) <= lax.broadcasted_iota(jnp.int32, (TOKS, TOKS), 1)).astype(F32).astype(BF)
    seen = jnp.zeros((8, 1), F32)
    starts = jnp.zeros((8, 128), F32)
    for b in range(blocks):
        at = b * TOKS
        table = tables[at // tok][:, at % tok : at % tok + TOKS]

        def both(i, other):
            return jnp.where(line < EXPERTS, table[i : i + 1], jnp.where(line < 2 * EXPERTS, table[i + 2 : i + 3], other))

        hit0 = both(0, -1.0) == target
        hit1 = both(1, -1.0) == target
        mask = jnp.where(hit0 | hit1, 1.0, 0.0)
        count = mm(mask.astype(BF), upto)
        slot = jnp.where(mask > 0.0, seen + count - 1.0, -1.0)
        gate = jnp.where(hit0, both(4, 0.0), 0.0) + jnp.where(hit1, both(5, 0.0), 0.0)
        choice = jnp.where(hit1, 1.0, 0.0)
        rows_ref[:, at : at + TOKS] = slot
        starts = jnp.where(lane == b, seen, starts)
        for layer, cols_ref in ((0, cols_a_ref), (1, cols_b_ref)):
            part = slice(layer * EXPERTS, (layer + 1) * EXPERTS)
            stack = jnp.concatenate([slot[part], gate[part], choice[part], choice[part]], axis=0)
            cols_ref[at : at + TOKS, :] = stack.T
        seen = seen + count[:, TOKS - 1 :]
    starts_ref[...] = jnp.where(lane == blocks, seen, starts).astype(jnp.int32)


def weight_copies(hbm, vmem, sems, e):
    return [pltpu.make_async_copy(h.at[e], v.at[e], sems.at[e, i]) for i, (h, v) in enumerate(zip(hbm, vmem))]


def forward_kernel(layer, starts_ref, x0, x1, x2, x3, rows_ref, cols_ref, w1_hbm, w3_hbm, w2_hbm,
                   y0, y1, y2, y3, w1, w3, w2, u_all, o_all, h_ref, y_buf, w_sems, y_sems):
    xs, ys = (x0, x1, x2, x3), (y0, y1, y2, y3)
    blocks = rows_ref.shape[1] // TOKS
    width = w1.shape[2]
    slots = Slots(layer, starts_ref, rows_ref, cols_ref, blocks)
    for e in range(EXPERTS):
        for copy in weight_copies((w1_hbm, w3_hbm, w2_hbm), (w1, w3, w2), w_sems, e):
            copy.start()

    def tokens_of(b):
        ref, toks = block_of(xs, b)
        return ref[toks, :]

    for e in range(EXPERTS):
        slots.compact(e, (tokens_of,), (u_all.at[e],))

    def expert(e, carry):
        for copy in weight_copies((w1_hbm, w3_hbm, w2_hbm), (w1, w3, w2), w_sems, e):
            copy.wait()

        def tile(k, inner):
            u = u_all[e, tile_rows(k), :]
            for c in range(0, width, COLS):
                cols = slice(c, c + COLS)
                a = mm(u, w1[e, :, cols])
                b = mm(u, w3[e, :, cols])
                h_ref[:, cols] = (a * jax.nn.sigmoid(a) * b).astype(BF)
            o_all[e, tile_rows(k), :] = mm(h_ref[...], w2[e]).astype(BF)
            return inner

        return lax.fori_loop(0, slots.tiles(e), tile, carry)

    lax.fori_loop(0, EXPERTS, expert, 0)
    for e in range(EXPERTS):
        slots.zero_after(e, o_all.at[e])
    copies = []
    for b in range(blocks):
        y_buf[b] = sum(slots.gate(e, b) * slots.spread(e, b, o_all.at[e]) for e in range(EXPERTS))
        ref, toks = block_of(ys, b)
        copies.append(pltpu.make_async_copy(y_buf.at[b], ref.at[toks, :], y_sems.at[b]))
        copies[-1].start()
    for copy in copies:
        copy.wait()


def dx_kernel(layer, starts_ref, x0, x1, x2, x3, g0, g1, g2, g3, rows_ref, cols_ref, w1_hbm, w3_hbm, w2_hbm,
              dx0, dx1, dx2, dx3, kept_hbm, w1, w3, w2, u_all, q_all, od_all, kept, dx_buf, dg_buf, w_sems, k_sems, dx_sems, dg_sems):
    xs, gs, dxs = (x0, x1, x2, x3), (g0, g1, g2, g3), (dx0, dx1, dx2, dx3)
    tok = x0.shape[0]
    blocks = rows_ref.shape[1] // TOKS
    dim, width = w1.shape[1:]
    slots = Slots(layer, starts_ref, rows_ref, cols_ref, blocks)
    for e in range(EXPERTS):
        for copy in weight_copies((w1_hbm, w3_hbm, w2_hbm), (w1, w3, w2), w_sems, e):
            copy.start()

    def tokens_of(b):
        ref, toks = block_of(xs, b)
        return ref[toks, :]

    for e in range(EXPERTS):

        def scaled_of(b):
            ref, toks = block_of(gs, b)
            return (slots.gate(e, b) * ref[toks, :].astype(F32)).astype(BF)

        slots.compact(e, (tokens_of, scaled_of), (u_all.at[e], q_all.at[e]))

    def copy_out(e, k):
        return pltpu.make_async_copy(kept.at[lax.rem(k, 2)], kept_hbm.at[e, tile_rows(k), :], k_sems.at[lax.rem(k, 2)])

    def expert(e, carry):
        for copy in weight_copies((w1_hbm, w3_hbm, w2_hbm), (w1, w3, w2), w_sems, e):
            copy.wait()
        count = slots.tiles(e)

        def tile(k, inner):
            slot = lax.rem(k, 2)

            @pl.when(k >= 2)
            def _():
                copy_out(e, k - 2).wait()

            u = u_all[e, tile_rows(k), :]
            q = q_all[e, tile_rows(k), :]
            for c in range(0, width, COLS):
                cols = slice(c, c + COLS)
                a = mm(u, w1[e, :, cols])
                b = mm(u, w3[e, :, cols])
                dh = mm_nt(q, w2[e, cols, :])
                s = jax.nn.sigmoid(a)
                act = a * s
                kept[slot, :, c : c + COLS] = (act * b).astype(BF)
                kept[slot, :, width + c : width + c + COLS] = (dh * b * s * (1.0 + a * (1.0 - s))).astype(BF)
                kept[slot, :, 2 * width + c : 2 * width + c + COLS] = (dh * act).astype(BF)
            kept[slot, :, 3 * width : 3 * width + dim] = u
            kept[slot, :, 3 * width + dim :] = q
            od_all[e, tile_rows(k), :dim] = mm(kept[slot, :, :width], w2[e]).astype(BF)
            du = mm_nt(kept[slot, :, width : 2 * width], w1[e]) + mm_nt(kept[slot, :, 2 * width : 3 * width], w3[e])
            od_all[e, tile_rows(k), dim:] = du.astype(BF)
            copy_out(e, k).start()
            return inner

        lax.fori_loop(0, count, tile, 0)

        @pl.when(count >= 2)
        def _():
            copy_out(e, count - 2).wait()

        @pl.when(count >= 1)
        def _():
            copy_out(e, count - 1).wait()

        return carry

    lax.fori_loop(0, EXPERTS, expert, 0)
    for e in range(EXPERTS):
        slots.zero_after(e, od_all.at[e])
    copies = []
    lane = lax.broadcasted_iota(jnp.int32, (TOKS, 8), 1).astype(F32)
    for b in range(blocks):
        gref, toks = block_of(gs, b)
        dy = gref[toks, :].astype(F32)
        dx = jnp.zeros((TOKS, dim), F32)
        dg = jnp.zeros((TOKS, 8), F32)
        for e in range(EXPERTS):
            od = slots.spread(e, b, od_all.at[e])
            dx += od[:, dim:]
            dg += jnp.where(lane == slots.choice(e, b), jnp.sum(dy * od[:, :dim], axis=1, keepdims=True), 0.0)
        dx_buf[b] = dx
        dg_buf[b * TOKS // tok, :, toks] = dg.T
        copies.append(pltpu.make_async_copy(dx_buf.at[b], block_of(dxs, b)[0].at[toks, :], dx_sems.at[b]))
        copies[-1].start()
    for i, dst in enumerate(dxs):
        copies.append(pltpu.make_async_copy(dg_buf.at[i], dst.at[tok : tok + 8, :], dg_sems.at[i]))
        copies[-1].start()
    for copy in copies:
        copy.wait()


def dw_kernel(layer, starts_ref, kept_hbm, dw1_hbm, dw3_hbm, dw2_hbm, kept, dw1, dw3, dw2, k_sems, o_sems):
    dim, width = dw1.shape[1:]
    blocks = kept_hbm.shape[1] // TOKS
    slots = Slots(layer, starts_ref, None, None, blocks)

    def copy_in(e, k, slot):
        return pltpu.make_async_copy(kept_hbm.at[e, tile_rows(k), :], kept.at[slot], k_sems.at[slot])

    def copy_out(e, i):
        return pltpu.make_async_copy((dw1, dw3, dw2)[i].at[e], (dw1_hbm, dw3_hbm, dw2_hbm)[i].at[e], o_sems.at[e, i])

    first_tiles = slots.tiles(0)
    count = first_tiles + slots.tiles(1)

    def where(g):
        e = (g >= first_tiles).astype(jnp.int32)
        return e, g - e * first_tiles

    copy_in(*where(0), 0).start()

    def tile(g, carry):
        slot = lax.rem(g, 2)
        e, k = where(g)
        copy_in(e, k, slot).wait()

        @pl.when(g + 1 < count)
        def _():
            copy_in(*where(g + 1), 1 - slot).start()

        u = kept[slot, :, 3 * width : 3 * width + dim]
        q = kept[slot, :, 3 * width + dim :]
        fresh = k == 0
        last = (g == first_tiles - 1) | (g == count - 1)

        def put(ref, index, part):
            ref[index] = jnp.where(fresh, part, ref[index] + part)

        def leave(i):
            pl.when(last)(lambda: copy_out(e, i).start())

        for c in range(0, width, COLS):
            put(dw1, (e, slice(None), slice(c, c + COLS)), mm_tn(u, kept[slot, :, width + c : width + c + COLS]))
        leave(0)
        for c in range(0, width, COLS):
            put(dw3, (e, slice(None), slice(c, c + COLS)), mm_tn(u, kept[slot, :, 2 * width + c : 2 * width + c + COLS]))
        leave(1)
        for c in range(0, width, COLS):
            put(dw2, (e, slice(c, c + COLS), slice(None)), mm_tn(kept[slot, :, c : c + COLS], q))
        leave(2)
        return carry

    lax.fori_loop(0, count, tile, 0)
    for e in range(EXPERTS):
        for i in range(3):
            copy_out(e, i).wait()


IN_VMEM = pl.BlockSpec(memory_space=pltpu.VMEM)
IN_SMEM = pl.BlockSpec(memory_space=pltpu.SMEM)
IN_HBM = pl.BlockSpec(memory_space=pl.ANY)


def call(kernel, layer, operands, in_specs, outs, out_specs, scratch, flops):
    return pl.pallas_call(
        lambda *refs: kernel(layer, *refs) if layer is not None else kernel(*refs),
        in_specs=in_specs,
        out_specs=out_specs,
        out_shape=outs,
        scratch_shapes=scratch,
        compiler_params=pltpu.CompilerParams(vmem_limit_bytes=VMEM),
        cost_estimate=pl.CostEstimate(flops=flops, bytes_accessed=40_000_000, transcendentals=0),
    )(*operands)


def run_routing(tables):
    tokens = tables[0].shape[1] * len(tables)
    rows, cols_a, cols_b, starts = call(
        routing_kernel, None, tables, [IN_VMEM] * 4,
        [
            jax.ShapeDtypeStruct((8, tokens), F32),
            jax.ShapeDtypeStruct((tokens, 8), F32),
            jax.ShapeDtypeStruct((tokens, 8), F32),
            jax.ShapeDtypeStruct((8, 128), jnp.int32),
        ],
        [IN_VMEM] * 4, [], 10_000_000,
    )
    return (starts, rows, cols_a), (starts, rows, cols_b)


def weight_scratch(w1, w2):
    return [pltpu.VMEM(w1.shape, BF), pltpu.VMEM(w1.shape, BF), pltpu.VMEM(w2.shape, BF)]


def run_forward(layer, xs, maps, w1, w3, w2):
    tok, dim = xs[0].shape
    tokens = tok * len(xs)
    width = w1.shape[2]
    blocks = tokens // TOKS
    most = tokens + SPAN + ROWS
    return call(
        forward_kernel, layer, (maps[0], *xs, maps[1], maps[2], w1, w3, w2),
        [IN_SMEM] + [IN_VMEM] * 6 + [IN_HBM] * 3,
        [jax.ShapeDtypeStruct((tok, dim), F32)] * 4,
        [IN_HBM] * 4,
        weight_scratch(w1, w2)
        + [pltpu.VMEM((EXPERTS, most, dim), BF)] * 2
        + [pltpu.VMEM((ROWS, width), BF), pltpu.VMEM((blocks, TOKS, dim), F32)]
        + [pltpu.SemaphoreType.DMA((EXPERTS, 3)), pltpu.SemaphoreType.DMA((blocks,))],
        2 * 3 * tokens * dim * width,
    )


def run_dx(layer, xs, gs, maps, w1, w3, w2):
    tok, dim = xs[0].shape
    tokens = tok * len(xs)
    width = w1.shape[2]
    blocks = tokens // TOKS
    most = tokens + SPAN + ROWS
    kept = 3 * width + 2 * dim
    out = call(
        dx_kernel, layer, (maps[0], *xs, *gs, maps[1], maps[2], w1, w3, w2),
        [IN_SMEM] + [IN_VMEM] * 10 + [IN_HBM] * 3,
        [jax.ShapeDtypeStruct((tok + 8, dim), F32)] * 4 + [jax.ShapeDtypeStruct((EXPERTS, tokens, kept), BF)],
        [IN_HBM] * 5,
        weight_scratch(w1, w2)
        + [pltpu.VMEM((EXPERTS, most, dim), BF)] * 2
        + [pltpu.VMEM((EXPERTS, most, 2 * dim), BF), pltpu.VMEM((2, ROWS, kept), BF), pltpu.VMEM((blocks, TOKS, dim), F32)]
        + [pltpu.VMEM((4, 8, tok), F32)]
        + [pltpu.SemaphoreType.DMA((EXPERTS, 3)), pltpu.SemaphoreType.DMA((2,)), pltpu.SemaphoreType.DMA((blocks,))]
        + [pltpu.SemaphoreType.DMA((4,))],
        2 * 6 * tokens * dim * width,
    )
    return out[:4], out[4]


def run_dw(layer, kept, maps, shape1, shape2):
    tokens = kept.shape[1]
    return call(
        dw_kernel, layer, (maps[0], kept),
        [IN_SMEM, IN_HBM],
        [jax.ShapeDtypeStruct(shape1, F32), jax.ShapeDtypeStruct(shape1, F32), jax.ShapeDtypeStruct(shape2, F32)],
        [IN_HBM] * 3,
        [pltpu.VMEM((2, ROWS, kept.shape[2]), BF), pltpu.VMEM(shape1, F32), pltpu.VMEM(shape1, F32), pltpu.VMEM(shape2, F32)]
        + [pltpu.SemaphoreType.DMA((2,)), pltpu.SemaphoreType.DMA((EXPERTS, 3))],
        2 * 3 * tokens * shape1[1] * shape1[2],
    )


def solution(mesh):
    tok_spec = P(("dp", "ep"))
    w_spec = P("ep")
    across = [(0, 2), (2, 0), (1, 3), (3, 1)]
    beside = [(0, 1), (1, 0), (2, 3), (3, 2)]
    cross = [(0, 3), (3, 0), (1, 2), (2, 1)]

    def permute(v, pairs):
        return lax.ppermute(v, "ep", pairs)

    def gather(own):
        other = permute(own, across)
        return other, permute(other, beside), own, permute(own, beside)

    def gather_direct(own):
        return permute(own, across), permute(own, cross), own, permute(own, beside)

    def combine(parts):
        other, diagonal, own, mate = parts
        theirs = other + permute(diagonal, beside)
        return own + permute(mate, beside) + permute(theirs, across)

    def device_program(x_in, idx_a, idx_b, gate_a, gate_b, dy_out, w1_a, w3_a, w2_a, w1_b, w3_b, w2_b):
        tok, top_k = idx_a.shape
        own_map = jnp.concatenate([idx_a.astype(F32), idx_b.astype(F32), gate_a, gate_b], axis=1).T
        maps_a, maps_b = run_routing(gather_direct(own_map))

        def add(base, total):
            return (base.astype(F32) + total[:tok]).astype(BF)

        def dgate_of(total):
            return total[tok : tok + top_k].T

        x_all = gather(x_in)
        dy_all = gather_direct(dy_out)
        x_mid = add(x_in, combine(run_forward(0, x_all, maps_a, w1_a, w3_a, w2_a)))
        mid_all = gather(x_mid)
        x_again, mid_other = lax.optimization_barrier((x_in, mid_all[0]))
        mid_all = (mid_other, *mid_all[1:])
        again_all = gather_direct(x_again)
        dx_parts, kept_b = run_dx(1, mid_all, dy_all, maps_b, w1_b, w3_b, w2_b)
        total = combine(dx_parts)
        dx_mid, dgate_b = add(dy_out, total), dgate_of(total)
        dmid_all = gather_direct(dx_mid)
        x_out = add(x_mid, combine(run_forward(1, mid_all, maps_b, w1_b, w3_b, w2_b)))
        grads_b = run_dw(1, kept_b, maps_b, w1_b.shape, w2_b.shape)
        dx_parts, kept_a = run_dx(0, again_all, dmid_all, maps_a, w1_a, w3_a, w2_a)
        total = combine(dx_parts)
        dx_in, dgate_a = add(dx_mid, total), dgate_of(total)
        grads_a = run_dw(0, kept_a, maps_a, w1_a.shape, w2_a.shape)
        return (x_out, dx_in, *grads_a, *grads_b, dgate_a, dgate_b)


    return jax.shard_map(device_program, mesh=mesh, in_specs=(tok_spec,) * 6 + (w_spec,) * 6, out_specs=(tok_spec,) * 10, check_vma=False)
```

```python
import functools

import jax
import jax.numpy as jnp
from jax import lax
from jax.experimental import pallas as pl
from jax.experimental.pallas import tpu as pltpu
from jax.sharding import PartitionSpec as P


ROWS = 256
TOKS = 128
WIDE = 2
SPAN = WIDE * TOKS + 16
COLS = 256
EXPERTS = 2
VMEM = 66_000_000

BF = jnp.bfloat16
F32 = jnp.float32


def mm(a, b):
    return lax.dot_general(a, b, (((1,), (0,)), ((), ())), preferred_element_type=F32)


def mm_nt(a, b):
    return lax.dot_general(a, b, (((1,), (1,)), ((), ())), preferred_element_type=F32)


def mm_tn(a, b):
    return lax.dot_general(a, b, (((0,), (0,)), ((), ())), preferred_element_type=F32)


def block_of(refs, b, wide=1):
    size = wide * TOKS
    per = refs[0].shape[0] // size
    return refs[b // per], slice((b % per) * size, (b % per + 1) * size)


def tile_rows(k):
    return pl.ds(pl.multiple_of(k * ROWS, ROWS), ROWS)


class Slots:
    def __init__(self, starts_ref, rows_ref, cols_ref, blocks):
        self.starts_ref, self.rows_ref, self.cols_ref, self.blocks = starts_ref, rows_ref, cols_ref, blocks

    def tiles(self, e):
        return (self.starts_ref[e, self.blocks] + ROWS - 1) // ROWS

    def base(self, e, b):
        return pl.multiple_of((self.starts_ref[e, b] // 16) * 16, 16)

    def col(self, b, i, wide=1):
        size = wide * TOKS
        return self.cols_ref[pl.ds(pl.multiple_of(b * size, size), size), i : i + 1]

    def gate(self, e, b, wide=1):
        if isinstance(e, int):
            return self.col(b, EXPERTS + e, wide)
        return jnp.where(e == 0, self.col(b, EXPERTS, wide), self.col(b, EXPERTS + 1, wide))

    def choice(self, e, b, wide=1):
        return self.col(b, 2 * EXPERTS + e, wide)

    def compact(self, e, makers, outs):
        size = WIDE * TOKS
        line = lax.broadcasted_iota(jnp.int32, (size + 16, size), 0).astype(F32)
        for b in range(self.blocks // WIDE):
            base = self.base(e, b * WIDE)
            slot = self.rows_ref[pl.ds(e, 1), b * size : (b + 1) * size] - base.astype(F32)
            hot = jnp.where(slot == line, 1.0, 0.0).astype(BF)
            for make, out in zip(makers, outs):
                rows = mm(hot, make(b)).astype(BF)
                if b == 0:
                    out[pl.ds(base, size + 16), :] = rows
                else:
                    out[pl.ds(base, 16), :] += rows[:16]
                    out[pl.ds(base + 16, size), :] = rows[16:]
        end = self.base(e, self.blocks - WIDE) + size + 16
        for out in outs:
            out[pl.ds(end, ROWS), :] = jnp.zeros((ROWS, out.shape[1]), BF)

    def spread(self, e, b, ref, wide=1):
        size = wide * TOKS
        base = self.base(e, b * wide)
        line = lax.broadcasted_iota(jnp.int32, (size, size + 16), 1).astype(F32)
        hot = jnp.where(self.col(b, e, wide) - base.astype(F32) == line, 1.0, 0.0).astype(BF)
        return mm(hot, ref[pl.ds(base, size + 16), :])

    def zero_after(self, e, ref):
        end = pl.multiple_of(self.tiles(e) * ROWS, ROWS)
        ref[pl.ds(end, SPAN), :] = jnp.zeros((SPAN, ref.shape[1]), BF)


def routing_kernel(t0, t1, t2, t3, *refs):
    tables = (t0, t1, t2, t3)
    full_a, full_b, halves = refs[0:3], refs[3:6], (refs[6:9], refs[9:12])
    tok = t0.shape[1]
    blocks = len(tables) * tok // TOKS
    half = blocks // 2
    first = (lax.axis_index("ep") * EXPERTS).astype(F32)
    line = lax.broadcasted_iota(jnp.int32, (8, TOKS), 0)
    target = first + (line % EXPERTS).astype(F32)
    lane = lax.broadcasted_iota(jnp.int32, (8, 128), 1)
    upto = (lax.broadcasted_iota(jnp.int32, (TOKS, TOKS), 0) <= lax.broadcasted_iota(jnp.int32, (TOKS, TOKS), 1)).astype(F32).astype(BF)
    seen = jnp.zeros((8, 1), F32)
    before = jnp.zeros((8, 1), F32)
    starts = jnp.zeros((8, 128), F32)
    later = jnp.zeros((8, 128), F32)
    for b in range(blocks):
        at = b * TOKS
        table = tables[at // tok][:, at % tok : at % tok + TOKS]
        if b == half:
            before = seen

        def both(i, other):
            return jnp.where(line < EXPERTS, table[i : i + 1], jnp.where(line < 2 * EXPERTS, table[i + 2 : i + 3], other))

        hit0 = both(0, -1.0) == target
        hit1 = both(1, -1.0) == target
        mask = jnp.where(hit0 | hit1, 1.0, 0.0)
        count = mm(mask.astype(BF), upto)
        slot = jnp.where(mask > 0.0, seen + count - 1.0, -1.0)
        part_slot = jnp.where(mask > 0.0, seen - before + count - 1.0, -1.0)
        gate = jnp.where(hit0, both(4, 0.0), 0.0) + jnp.where(hit1, both(5, 0.0), 0.0)
        choice = jnp.where(hit1, 1.0, 0.0)
        starts = jnp.where(lane == b, seen, starts)
        if b >= half:
            later = jnp.where(lane == b - half, seen - before, later)

        def put(outs, layer, here, slots):
            part = slice(layer * EXPERTS, (layer + 1) * EXPERTS)
            outs[1][:, here : here + TOKS] = slots[part]
            stack = jnp.concatenate([slots[part], gate[part], choice[part], choice[part]], axis=0)
            outs[2][here : here + TOKS, :] = stack.T

        put(full_a, 0, at, slot)
        put(full_b, 1, at, slot)
        put(halves[b // half], 0, at % (half * TOKS), part_slot)
        seen = seen + count[:, TOKS - 1 :]
    starts = jnp.where(lane == blocks, seen, starts).astype(jnp.int32)
    later = jnp.where(lane == half, seen - before, later).astype(jnp.int32)
    full_a[0][...] = starts[:EXPERTS]
    full_b[0][...] = starts[EXPERTS : 2 * EXPERTS]
    halves[0][0][...] = starts[:EXPERTS]
    halves[1][0][...] = later[:EXPERTS]


def weight_copies(hbm, vmem, sems, e):
    return [pltpu.make_async_copy(h.at[e], v.at[e], sems.at[e, i]) for i, (h, v) in enumerate(zip(hbm, vmem))]


def forward_kernel(n, starts_ref, *refs):
    xs, (rows_ref, cols_ref, w1_hbm, w3_hbm, w2_hbm), ys = refs[:n], refs[n : n + 5], refs[n + 5 : 2 * n + 5]
    w1, w3, w2, u_all, o_all, h_ref, y_buf, w_sems, y_sems = refs[2 * n + 5 :]
    blocks = rows_ref.shape[1] // TOKS
    width = w1.shape[2]
    slots = Slots(starts_ref, rows_ref, cols_ref, blocks)
    for e in range(EXPERTS):
        for copy in weight_copies((w1_hbm, w3_hbm, w2_hbm), (w1, w3, w2), w_sems, e):
            copy.start()

    def tokens_of(b):
        ref, toks = block_of(xs, b, WIDE)
        return ref[toks, :]

    def gather_rows(e, carry):
        slots.compact(e, (tokens_of,), (u_all.at[e],))
        return carry

    lax.fori_loop(0, EXPERTS, gather_rows, 0)

    def expert(e, carry):
        for copy in weight_copies((w1_hbm, w3_hbm, w2_hbm), (w1, w3, w2), w_sems, e):
            copy.wait()

        def tile(k, inner):
            u = u_all[e, tile_rows(k), :]
            for c in range(0, width, COLS):
                cols = slice(c, c + COLS)
                a = mm(u, w1[e, :, cols])
                b = mm(u, w3[e, :, cols])
                h_ref[:, cols] = (a * jax.nn.sigmoid(a) * b).astype(BF)
            o_all[e, tile_rows(k), :] = mm(h_ref[...], w2[e]).astype(BF)
            return inner

        return lax.fori_loop(0, slots.tiles(e), tile, carry)

    lax.fori_loop(0, EXPERTS, expert, 0)
    for e in range(EXPERTS):
        slots.zero_after(e, o_all.at[e])
    copies = []
    each = ys[0].shape[0] // TOKS
    for i, ref in enumerate(ys):

        def blocks_of(half, carry):
            for step in range(each // 2):
                j = half * (each // 2) + step
                b = i * each + j
                toks = pl.ds(pl.multiple_of(j * TOKS, TOKS), TOKS)
                y_buf[i, toks, :] = sum(slots.gate(e, b) * slots.spread(e, b, o_all.at[e]) for e in range(EXPERTS))
            return carry

        lax.fori_loop(0, 2, blocks_of, 0)
        copies.append(pltpu.make_async_copy(y_buf.at[i], ref, y_sems.at[i]))
        copies[-1].start()
    for copy in copies:
        copy.wait()


def dx_kernel(starts_ref, x0, x1, x2, x3, g0, g1, g2, g3, rows_ref, cols_ref, w1_hbm, w3_hbm, w2_hbm,
              dx0, dx1, dx2, dx3, kept_hbm, w1, w3, w2, u_all, q_all, od_all, kept, dx_buf, w_sems, k_sems, dx_sems):
    xs, gs, dxs = (x0, x1, x2, x3), (g0, g1, g2, g3), (dx0, dx1, dx2, dx3)
    tok = x0.shape[0]
    blocks = rows_ref.shape[1] // TOKS
    dim, width = w1.shape[1:]
    slots = Slots(starts_ref, rows_ref, cols_ref, blocks)
    for e in range(EXPERTS):
        for copy in weight_copies((w1_hbm, w3_hbm, w2_hbm), (w1, w3, w2), w_sems, e):
            copy.start()

    def tokens_of(b):
        ref, toks = block_of(xs, b, WIDE)
        return ref[toks, :]

    def gather_rows(e, carry):
        def scaled_of(b):
            ref, toks = block_of(gs, b, WIDE)
            return (slots.gate(e, b, WIDE) * ref[toks, :].astype(F32)).astype(BF)

        slots.compact(e, (tokens_of, scaled_of), (u_all.at[e], q_all.at[e]))
        return carry

    lax.fori_loop(0, EXPERTS, gather_rows, 0)

    def copy_out(e, k):
        return pltpu.make_async_copy(kept.at[lax.rem(k, 2)], kept_hbm.at[e, tile_rows(k), :], k_sems.at[lax.rem(k, 2)])

    def expert(e, carry):
        for copy in weight_copies((w1_hbm, w3_hbm, w2_hbm), (w1, w3, w2), w_sems, e):
            copy.wait()
        count = slots.tiles(e)

        def tile(k, inner):
            slot = lax.rem(k, 2)

            @pl.when(k >= 2)
            def _():
                copy_out(e, k - 2).wait()

            u = u_all[e, tile_rows(k), :]
            q = q_all[e, tile_rows(k), :]
            for c in range(0, width, COLS):
                cols = slice(c, c + COLS)
                a = mm(u, w1[e, :, cols])
                b = mm(u, w3[e, :, cols])
                dh = mm_nt(q, w2[e, cols, :])
                s = jax.nn.sigmoid(a)
                act = a * s
                kept[slot, :, c : c + COLS] = (act * b).astype(BF)
                kept[slot, :, width + c : width + c + COLS] = (dh * b * s * (1.0 + a * (1.0 - s))).astype(BF)
                kept[slot, :, 2 * width + c : 2 * width + c + COLS] = (dh * act).astype(BF)
            kept[slot, :, 3 * width : 3 * width + dim] = u
            kept[slot, :, 3 * width + dim :] = q
            od_all[e, tile_rows(k), :dim] = mm(kept[slot, :, :width], w2[e]).astype(BF)
            du = mm_nt(kept[slot, :, width : 2 * width], w1[e]) + mm_nt(kept[slot, :, 2 * width : 3 * width], w3[e])
            od_all[e, tile_rows(k), dim:] = du.astype(BF)
            copy_out(e, k).start()
            return inner

        lax.fori_loop(0, count, tile, 0)

        @pl.when(count >= 2)
        def _():
            copy_out(e, count - 2).wait()

        @pl.when(count >= 1)
        def _():
            copy_out(e, count - 1).wait()

        return carry

    lax.fori_loop(0, EXPERTS, expert, 0)
    for e in range(EXPERTS):
        slots.zero_after(e, od_all.at[e])
    copies = []
    size = WIDE * TOKS
    each = tok // size
    lane = lax.broadcasted_iota(jnp.int32, (size, 8), 1).astype(F32)
    for i, ref in enumerate(dxs):

        for j in range(each):
            b = i * each + j
            toks = slice(j * size, (j + 1) * size)
            dy = gs[i][toks, :].astype(F32)
            dx = jnp.zeros((size, dim), F32)
            dg = jnp.zeros((size, 8), F32)
            for e in range(EXPERTS):
                od = slots.spread(e, b, od_all.at[e], WIDE)
                dx += od[:, dim:]
                dg += jnp.where(lane == slots.choice(e, b, WIDE), jnp.sum(dy * od[:, :dim], axis=1, keepdims=True), 0.0)
            dx_buf[i, toks, :] = dx
            dx_buf[i, tok : tok + 8, toks] = dg.T
        copies.append(pltpu.make_async_copy(dx_buf.at[i], ref, dx_sems.at[i]))
        copies[-1].start()
    for copy in copies:
        copy.wait()


def dw_kernel(starts_ref, kept_hbm, dw1_hbm, dw3_hbm, dw2_hbm, kept, dw1, dw3, dw2, k_sems, o_sems):
    dim, width = dw1.shape[1:]
    slots = Slots(starts_ref, None, None, kept_hbm.shape[1] // TOKS)

    def copy_in(e, k, slot):
        rows = pl.ds(pl.multiple_of(k * 2 * ROWS, 2 * ROWS), 2 * ROWS)
        return pltpu.make_async_copy(kept_hbm.at[e, rows, :], kept.at[slot], k_sems.at[slot])

    def copy_out(e, i):
        return pltpu.make_async_copy((dw1, dw3, dw2)[i].at[e], (dw1_hbm, dw3_hbm, dw2_hbm)[i].at[e], o_sems.at[e, i])

    first_tiles = (slots.tiles(0) + 1) // 2
    count = first_tiles + (slots.tiles(1) + 1) // 2

    def where(g):
        e = (g >= first_tiles).astype(jnp.int32)
        return e, g - e * first_tiles

    copy_in(*where(0), 0).start()

    def tile(g, carry):
        slot = lax.rem(g, 2)
        e, k = where(g)
        copy_in(e, k, slot).wait()

        @pl.when(g + 1 < count)
        def _():
            copy_in(*where(g + 1), 1 - slot).start()

        @pl.when(2 * k + 1 == slots.tiles(e))
        def _():
            kept[slot, ROWS:, :] = jnp.zeros((ROWS, kept.shape[2]), BF)

        u = kept[slot, :, 3 * width : 3 * width + dim]
        q = kept[slot, :, 3 * width + dim :]
        fresh = k == 0
        last = (g == first_tiles - 1) | (g == count - 1)

        def put(ref, index, part):
            ref[index] = jnp.where(fresh, part, ref[index] + part)

        def leave(i):
            pl.when(last)(lambda: copy_out(e, i).start())

        for c in range(0, width, COLS):
            put(dw1, (e, slice(None), slice(c, c + COLS)), mm_tn(u, kept[slot, :, width + c : width + c + COLS]))
        leave(0)
        for c in range(0, width, COLS):
            put(dw3, (e, slice(None), slice(c, c + COLS)), mm_tn(u, kept[slot, :, 2 * width + c : 2 * width + c + COLS]))
        leave(1)
        for c in range(0, width, COLS):
            put(dw2, (e, slice(c, c + COLS), slice(None)), mm_tn(kept[slot, :, c : c + COLS], q))
        leave(2)
        return carry

    lax.fori_loop(0, count, tile, 0)
    for e in range(EXPERTS):
        for i in range(3):
            copy_out(e, i).wait()


IN_VMEM = pl.BlockSpec(memory_space=pltpu.VMEM)
IN_SMEM = pl.BlockSpec(memory_space=pltpu.SMEM)
IN_HBM = pl.BlockSpec(memory_space=pl.ANY)


def call(kernel, operands, in_specs, outs, out_specs, scratch, flops):
    return pl.pallas_call(
        kernel,
        in_specs=in_specs,
        out_specs=out_specs,
        out_shape=outs,
        scratch_shapes=scratch,
        compiler_params=pltpu.CompilerParams(vmem_limit_bytes=VMEM),
        cost_estimate=pl.CostEstimate(flops=flops, bytes_accessed=40_000_000, transcendentals=0),
    )(*operands)


def run_routing(tables):
    tokens = tables[0].shape[1] * len(tables)
    outs = []
    for size in (tokens, tokens, tokens // 2, tokens // 2):
        outs.append(jax.ShapeDtypeStruct((EXPERTS, 128), jnp.int32))
        outs.append(jax.ShapeDtypeStruct((EXPERTS, size), F32))
        outs.append(jax.ShapeDtypeStruct((size, 8), F32))
    maps = call(routing_kernel, tables, [IN_VMEM] * 4, outs, [IN_VMEM] * 12, [], 10_000_000)
    return maps[0:3], maps[3:6], maps[6:9], maps[9:12]


def weight_scratch(w1, w2):
    return [pltpu.VMEM(w1.shape, BF), pltpu.VMEM(w1.shape, BF), pltpu.VMEM(w2.shape, BF)]


def run_forward(xs, maps, w1, w3, w2):
    tok, dim = xs[0].shape
    tokens = tok * len(xs)
    width = w1.shape[2]
    most = tokens + SPAN + ROWS
    return call(
        functools.partial(forward_kernel, len(xs)), (maps[0], *xs, maps[1], maps[2], w1, w3, w2),
        [IN_SMEM] + [IN_VMEM] * (len(xs) + 2) + [IN_HBM] * 3,
        [jax.ShapeDtypeStruct((tok, dim), F32)] * len(xs),
        [IN_HBM] * len(xs),
        weight_scratch(w1, w2)
        + [pltpu.VMEM((EXPERTS, most, dim), BF)] * 2
        + [pltpu.VMEM((ROWS, width), BF), pltpu.VMEM((len(xs), tok, dim), F32)]
        + [pltpu.SemaphoreType.DMA((EXPERTS, 3)), pltpu.SemaphoreType.DMA((len(xs),))],
        2 * 3 * tokens * dim * width,
    )


def run_dx(xs, gs, maps, w1, w3, w2):
    tok, dim = xs[0].shape
    tokens = tok * len(xs)
    width = w1.shape[2]
    most = tokens + SPAN + ROWS
    kept = 3 * width + 2 * dim
    out = call(
        dx_kernel, (maps[0], *xs, *gs, maps[1], maps[2], w1, w3, w2),
        [IN_SMEM] + [IN_VMEM] * 10 + [IN_HBM] * 3,
        [jax.ShapeDtypeStruct((tok + 8, dim), F32)] * 4 + [jax.ShapeDtypeStruct((EXPERTS, tokens, kept), BF)],
        [IN_HBM] * 5,
        weight_scratch(w1, w2)
        + [pltpu.VMEM((EXPERTS, most, dim), BF)] * 2
        + [pltpu.VMEM((EXPERTS, most, 2 * dim), BF), pltpu.VMEM((2, ROWS, kept), BF), pltpu.VMEM((4, tok + 8, dim), F32)]
        + [pltpu.SemaphoreType.DMA((EXPERTS, 3)), pltpu.SemaphoreType.DMA((2,)), pltpu.SemaphoreType.DMA((4,))],
        2 * 6 * tokens * dim * width,
    )
    return out[:4], out[4]


def run_dw(kept, maps, shape1, shape2):
    tokens = kept.shape[1]
    return call(
        dw_kernel, (maps[0], kept),
        [IN_SMEM, IN_HBM],
        [jax.ShapeDtypeStruct(shape1, F32), jax.ShapeDtypeStruct(shape1, F32), jax.ShapeDtypeStruct(shape2, F32)],
        [IN_HBM] * 3,
        [pltpu.VMEM((2, 2 * ROWS, kept.shape[2]), BF), pltpu.VMEM(shape1, F32), pltpu.VMEM(shape1, F32), pltpu.VMEM(shape2, F32)]
        + [pltpu.SemaphoreType.DMA((2,)), pltpu.SemaphoreType.DMA((EXPERTS, 3))],
        2 * 3 * tokens * shape1[1] * shape1[2],
    )


def solution(mesh):
    tok_spec = P(("dp", "ep"))
    w_spec = P("ep")
    across = [(0, 2), (2, 0), (1, 3), (3, 1)]
    beside = [(0, 1), (1, 0), (2, 3), (3, 2)]
    cross = [(0, 3), (3, 0), (1, 2), (2, 1)]

    def permute(v, pairs):
        return lax.ppermute(v, "ep", pairs)

    def gather(own):
        other = permute(own, across)
        return other, permute(other, beside), own, permute(own, beside)

    def gather_direct(own):
        return permute(own, across), permute(own, cross), own, permute(own, beside)

    def combine(parts):
        other, diagonal, own, mate = parts
        theirs = other + permute(diagonal, beside)
        return own + permute(mate, beside) + permute(theirs, across)

    def device_program(x_in, idx_a, idx_b, gate_a, gate_b, dy_out, w1_a, w3_a, w2_a, w1_b, w3_b, w2_b):
        tok, top_k = idx_a.shape
        own_map = jnp.concatenate([idx_a.astype(F32), idx_b.astype(F32), gate_a, gate_b], axis=1).T
        maps_a, maps_b, maps_far, maps_near = run_routing(gather_direct(own_map))

        def add(base, total):
            return (base.astype(F32) + total[:tok]).astype(BF)

        def dgate_of(total):
            return total[tok : tok + top_k].T

        x_all = gather(x_in)
        dy_all = gather(dy_out)
        far_parts = run_forward(x_all[:2], maps_far, w1_a, w3_a, w2_a)
        near_parts = run_forward(x_all[2:], maps_near, w1_a, w3_a, w2_a)
        x_mid = add(x_in, combine((*far_parts, *near_parts)))
        mid_all = gather(x_mid)
        x_again, mid_other = lax.optimization_barrier((x_in, mid_all[0]))
        mid_all = (mid_other, *mid_all[1:])
        again_all = gather_direct(x_again)
        dx_parts, kept_b = run_dx(mid_all, dy_all, maps_b, w1_b, w3_b, w2_b)
        total = combine(dx_parts)
        dx_mid, dgate_b = add(dy_out, total), dgate_of(total)
        dmid_all = gather_direct(dx_mid)
        x_out = add(x_mid, combine(run_forward(mid_all, maps_b, w1_b, w3_b, w2_b)))
        grads_b = run_dw(kept_b, maps_b, w1_b.shape, w2_b.shape)
        dx_parts, kept_a = run_dx(again_all, dmid_all, maps_a, w1_a, w3_a, w2_a)
        total = combine(dx_parts)
        dx_in, dgate_a = add(dx_mid, total), dgate_of(total)
        grads_a = run_dw(kept_a, maps_a, w1_a.shape, w2_a.shape)
        return (x_out, dx_in, *grads_a, *grads_b, dgate_a, dgate_b)


    return jax.shard_map(device_program, mesh=mesh, in_specs=(tok_spec,) * 6 + (w_spec,) * 6, out_specs=(tok_spec,) * 10, check_vma=False)
```

```python
import functools

import jax
import jax.numpy as jnp
from jax import lax
from jax.experimental import pallas as pl
from jax.experimental.pallas import tpu as pltpu
from jax.sharding import PartitionSpec as P


ROWS = 256
TOKS = 256
ALIGN = 16
COLS = 256
EXPERTS = 2
VMEM = 66_000_000

BF = jnp.bfloat16
F32 = jnp.float32


def mm(a, b):
    return lax.dot_general(a, b, (((1,), (0,)), ((), ())), preferred_element_type=F32)


def mm_nt(a, b):
    return lax.dot_general(a, b, (((1,), (1,)), ((), ())), preferred_element_type=F32)


def mm_tn(a, b):
    return lax.dot_general(a, b, (((0,), (0,)), ((), ())), preferred_element_type=F32)


def block_of(refs, b):
    per = refs[0].shape[0] // TOKS
    return refs[b // per], slice((b % per) * TOKS, (b % per + 1) * TOKS)


def tile_rows(k):
    return pl.ds(pl.multiple_of(k * ROWS, ROWS), ROWS)


class Slots:
    def __init__(self, starts_ref, rows_ref, cols_ref, blocks):
        self.starts_ref, self.rows_ref, self.cols_ref, self.blocks = starts_ref, rows_ref, cols_ref, blocks

    def tiles(self, e):
        return (self.starts_ref[e, self.blocks] + ROWS - 1) // ROWS

    def rows(self, e, b):
        return pl.ds(pl.multiple_of(self.starts_ref[e, b], ALIGN), TOKS)

    def base(self, e, b):
        return self.starts_ref[e, b].astype(F32)

    def col(self, b, i):
        return self.cols_ref[b * TOKS : (b + 1) * TOKS, i : i + 1]

    def gate(self, e, b):
        if isinstance(e, int):
            return self.col(b, EXPERTS + e)
        return jnp.where(e == 0, self.col(b, EXPERTS), self.col(b, EXPERTS + 1))

    def choice(self, e, b):
        return self.col(b, 2 * EXPERTS + e)

    def compact(self, e, makers, outs):
        line = lax.broadcasted_iota(jnp.int32, (TOKS, TOKS), 0).astype(F32)
        for b in range(self.blocks):
            slot = self.rows_ref[pl.ds(e, 1), b * TOKS : (b + 1) * TOKS] - self.base(e, b)
            hot = jnp.where(slot == line, 1.0, 0.0).astype(BF)
            for make, out in zip(makers, outs):
                out[self.rows(e, b), :] = mm(hot, make(b)).astype(BF)
        end = pl.multiple_of(self.starts_ref[e, self.blocks - 1] + TOKS, ALIGN)
        for out in outs:
            out[pl.ds(end, ROWS), :] = jnp.zeros((ROWS, out.shape[1]), BF)

    def spread(self, e, b, ref, more=0):
        line = lax.broadcasted_iota(jnp.int32, (TOKS, TOKS + more), 1).astype(F32)
        hot = jnp.where(self.col(b, e) - self.base(e, b) == line, 1.0, 0.0).astype(BF)
        rows = pl.ds(pl.multiple_of(self.starts_ref[e, b], ALIGN), TOKS + more)
        return mm(hot, ref[rows, :])

    def zero_after(self, e, ref):
        end = pl.multiple_of(self.tiles(e) * ROWS, ROWS)
        ref[pl.ds(end, TOKS + ALIGN), :] = jnp.zeros((TOKS + ALIGN, ref.shape[1]), BF)


def find_slots(tables, refs):
    full_a, full_b, halves = refs[0:3], refs[3:6], (refs[6:9], refs[9:12])
    tok = tables[0].shape[1]
    blocks = len(tables) * tok // TOKS
    half = blocks // 2
    first = (lax.axis_index("ep") * EXPERTS).astype(F32)
    line = lax.broadcasted_iota(jnp.int32, (8, TOKS), 0)
    target = first + (line % EXPERTS).astype(F32)
    lane = lax.broadcasted_iota(jnp.int32, (8, 128), 1)
    upto = (lax.broadcasted_iota(jnp.int32, (TOKS, TOKS), 0) <= lax.broadcasted_iota(jnp.int32, (TOKS, TOKS), 1)).astype(F32).astype(BF)
    seen = jnp.zeros((8, 1), F32)
    before = jnp.zeros((8, 1), F32)
    starts = jnp.zeros((8, 128), F32)
    later = jnp.zeros((8, 128), F32)
    for b in range(blocks):
        at = b * TOKS
        table = tables[at // tok][:, at % tok : at % tok + TOKS]
        if b == half:
            before = seen

        def both(i, other):
            return jnp.where(line < EXPERTS, table[i : i + 1], jnp.where(line < 2 * EXPERTS, table[i + 2 : i + 3], other))

        hit0 = both(0, -1.0) == target
        hit1 = both(1, -1.0) == target
        mask = jnp.where(hit0 | hit1, 1.0, 0.0)
        count = mm(mask.astype(BF), upto)
        slot = jnp.where(mask > 0.0, seen + count - 1.0, -1.0)
        part_slot = jnp.where(mask > 0.0, seen - before + count - 1.0, -1.0)
        gate = jnp.where(hit0, both(4, 0.0), 0.0) + jnp.where(hit1, both(5, 0.0), 0.0)
        choice = jnp.where(hit1, 1.0, 0.0)
        starts = jnp.where(lane == b, seen, starts)
        if b >= half:
            later = jnp.where(lane == b - half, seen - before, later)

        def put(outs, layer, here, slots):
            part = slice(layer * EXPERTS, (layer + 1) * EXPERTS)
            outs[1][:, here : here + TOKS] = slots[part]
            stack = jnp.concatenate([slots[part], gate[part], choice[part], choice[part]], axis=0)
            outs[2][here : here + TOKS, :] = stack.T

        put(full_a, 0, at, slot)
        put(full_b, 1, at, slot)
        put(halves[b // half], 0, at % (half * TOKS), part_slot)
        seen = seen + jnp.floor((count[:, TOKS - 1 :] + (ALIGN - 1.0)) / ALIGN) * ALIGN
    starts = jnp.where(lane == blocks, seen, starts).astype(jnp.int32)
    later = jnp.where(lane == half, seen - before, later).astype(jnp.int32)
    full_a[0][...] = starts[:EXPERTS]
    full_b[0][...] = starts[EXPERTS : 2 * EXPERTS]
    halves[0][0][...] = starts[:EXPERTS]
    halves[1][0][...] = later[:EXPERTS]


def gather_kernel(map_ref, x_ref, other_hbm, diagonal_hbm, mate_hbm, *refs):
    slot_refs, (maps, held, map_send, map_recv, far_send, far_recv, hop_send, hop_recv, near_send, near_recv, out_sems) = refs[:12], refs[12:]
    me = lax.axis_index("ep")
    mate = me + 1 - 2 * lax.rem(me, 2)
    other = lax.rem(me + 2, 4)
    diagonal = lax.rem(mate + 2, 4)
    pieces = far_send.shape[0]
    size = x_ref.shape[0] // pieces

    def send(src, dst, send_sem, recv_sem, to):
        return pltpu.make_async_remote_copy(
            src_ref=src, dst_ref=dst, send_sem=send_sem, recv_sem=recv_sem,
            device_id={"ep": to}, device_id_type=pl.DeviceIdType.MESH,
        )

    barrier = pltpu.get_barrier_semaphore()
    for peer in (other, diagonal, mate):
        pl.semaphore_signal(barrier, inc=1, device_id={"ep": peer}, device_id_type=pl.DeviceIdType.MESH)
    pl.semaphore_wait(barrier, 3)

    map_copies = [send(map_ref, maps.at[i], map_send.at[i], map_recv.at[i], to) for i, to in enumerate((other, diagonal, mate))]
    for copy in map_copies:
        copy.start()
    part = [pl.ds(p * size, size) for p in range(pieces)]
    far = [send(x_ref.at[part[p], :], held.at[0, part[p], :], far_send.at[p], far_recv.at[p], other) for p in range(pieces)]
    for copy in far:
        copy.start()
    near = send(x_ref, held.at[2], near_send, near_recv, mate)
    near.start()
    for copy in map_copies:
        copy.wait_recv()
    find_slots((maps.at[0], maps.at[1], map_ref, maps.at[2]), slot_refs)
    near.wait()
    outs = [pltpu.make_async_copy(held.at[2], mate_hbm, out_sems.at[2 * pieces])]
    outs[0].start()
    hops = []
    for p in range(pieces):
        far[p].wait_recv()
        hops.append(send(held.at[0, part[p], :], held.at[1, part[p], :], hop_send.at[p], hop_recv.at[p], mate))
        hops[p].start()
        outs.append(pltpu.make_async_copy(held.at[0, part[p], :], other_hbm.at[part[p], :], out_sems.at[p]))
        outs[-1].start()
    for p in range(pieces):
        hops[p].wait_recv()
        outs.append(pltpu.make_async_copy(held.at[1, part[p], :], diagonal_hbm.at[part[p], :], out_sems.at[pieces + p]))
        outs[-1].start()
    for copy in map_copies + far + hops:
        copy.wait_send()
    for copy in outs:
        copy.wait()


def weight_copies(hbm, vmem, sems, e):
    return [pltpu.make_async_copy(h.at[e], v.at[e], sems.at[e, i]) for i, (h, v) in enumerate(zip(hbm, vmem))]


def forward_kernel(n, starts_ref, *refs):
    xs, (rows_ref, cols_ref, w1_hbm, w3_hbm, w2_hbm), ys = refs[:n], refs[n : n + 5], refs[n + 5 : 2 * n + 5]
    w1, w3, w2, u_all, o_all, h_ref, y_buf, w_sems, y_sems = refs[2 * n + 5 :]
    blocks = rows_ref.shape[1] // TOKS
    width = w1.shape[2]
    slots = Slots(starts_ref, rows_ref, cols_ref, blocks)
    for e in range(EXPERTS):
        for copy in weight_copies((w1_hbm, w3_hbm, w2_hbm), (w1, w3, w2), w_sems, e):
            copy.start()

    def tokens_of(b):
        ref, toks = block_of(xs, b)
        return ref[toks, :]

    def gather_rows(e, carry):
        slots.compact(e, (tokens_of,), (u_all.at[e],))
        return carry

    lax.fori_loop(0, EXPERTS, gather_rows, 0)

    def expert(e, carry):
        for copy in weight_copies((w1_hbm, w3_hbm, w2_hbm), (w1, w3, w2), w_sems, e):
            copy.wait()

        def tile(k, inner):
            u = u_all[e, tile_rows(k), :]
            for c in range(0, width, COLS):
                cols = slice(c, c + COLS)
                a = mm(u, w1[e, :, cols])
                b = mm(u, w3[e, :, cols])
                h_ref[:, cols] = (a * jax.nn.sigmoid(a) * b).astype(BF)
            o_all[e, tile_rows(k), :] = mm(h_ref[...], w2[e]).astype(BF)
            return inner

        return lax.fori_loop(0, slots.tiles(e), tile, carry)

    lax.fori_loop(0, EXPERTS, expert, 0)
    for e in range(EXPERTS):
        slots.zero_after(e, o_all.at[e])
    copies = []
    each = ys[0].shape[0] // TOKS
    for i, ref in enumerate(ys):

        for j in range(each):
            b = i * each + j
            toks = slice(j * TOKS, (j + 1) * TOKS)
            y_buf[i, toks, :] = sum(slots.gate(e, b) * slots.spread(e, b, o_all.at[e]) for e in range(EXPERTS))
        copies.append(pltpu.make_async_copy(y_buf.at[i], ref, y_sems.at[i]))
        copies[-1].start()
    for copy in copies:
        copy.wait()


def dx_kernel(starts_ref, x0, x1, x2, x3, g0, g1, g2, g3, rows_ref, cols_ref, w1_hbm, w3_hbm, w2_hbm,
              dx0, dx1, dx2, dx3, kept_hbm, w1, w3, w2, u_all, q_all, od_all, kept, dx_buf, w_sems, k_sems, dx_sems):
    xs, gs, dxs = (x0, x1, x2, x3), (g0, g1, g2, g3), (dx0, dx1, dx2, dx3)
    tok = x0.shape[0]
    blocks = rows_ref.shape[1] // TOKS
    dim, width = w1.shape[1:]
    slots = Slots(starts_ref, rows_ref, cols_ref, blocks)
    for e in range(EXPERTS):
        for copy in weight_copies((w1_hbm, w3_hbm, w2_hbm), (w1, w3, w2), w_sems, e):
            copy.start()

    def tokens_of(b):
        ref, toks = block_of(xs, b)
        return ref[toks, :]

    def gather_rows(e, carry):
        def scaled_of(b):
            ref, toks = block_of(gs, b)
            return (slots.gate(e, b) * ref[toks, :].astype(F32)).astype(BF)

        slots.compact(e, (tokens_of, scaled_of), (u_all.at[e], q_all.at[e]))
        return carry

    lax.fori_loop(0, EXPERTS, gather_rows, 0)

    def copy_out(e, k):
        return pltpu.make_async_copy(kept.at[lax.rem(k, 2)], kept_hbm.at[e, tile_rows(k), :], k_sems.at[lax.rem(k, 2)])

    def expert(e, carry):
        for copy in weight_copies((w1_hbm, w3_hbm, w2_hbm), (w1, w3, w2), w_sems, e):
            copy.wait()
        count = slots.tiles(e)

        def tile(k, inner):
            slot = lax.rem(k, 2)

            @pl.when(k >= 2)
            def _():
                copy_out(e, k - 2).wait()

            u = u_all[e, tile_rows(k), :]
            q = q_all[e, tile_rows(k), :]
            for c in range(0, width, COLS):
                cols = slice(c, c + COLS)
                a = mm(u, w1[e, :, cols])
                b = mm(u, w3[e, :, cols])
                dh = mm_nt(q, w2[e, cols, :])
                s = jax.nn.sigmoid(a)
                act = a * s
                kept[slot, :, c : c + COLS] = (act * b).astype(BF)
                kept[slot, :, width + c : width + c + COLS] = (dh * b * s * (1.0 + a * (1.0 - s))).astype(BF)
                kept[slot, :, 2 * width + c : 2 * width + c + COLS] = (dh * act).astype(BF)
            kept[slot, :, 3 * width : 3 * width + dim] = u
            kept[slot, :, 3 * width + dim :] = q
            od_all[e, tile_rows(k), :dim] = mm(kept[slot, :, :width], w2[e]).astype(BF)
            du = mm_nt(kept[slot, :, width : 2 * width], w1[e]) + mm_nt(kept[slot, :, 2 * width : 3 * width], w3[e])
            od_all[e, tile_rows(k), dim:] = du.astype(BF)
            copy_out(e, k).start()
            return inner

        lax.fori_loop(0, count, tile, 0)

        @pl.when(count >= 2)
        def _():
            copy_out(e, count - 2).wait()

        @pl.when(count >= 1)
        def _():
            copy_out(e, count - 1).wait()

        return carry

    lax.fori_loop(0, EXPERTS, expert, 0)
    for e in range(EXPERTS):
        slots.zero_after(e, od_all.at[e])
    copies = []
    each = tok // TOKS
    lane = lax.broadcasted_iota(jnp.int32, (TOKS, 8), 1).astype(F32)
    for i, ref in enumerate(dxs):

        for j in range(each):
            b = i * each + j
            toks = slice(j * TOKS, (j + 1) * TOKS)
            dy = gs[i][toks, :].astype(F32)
            dx = jnp.zeros((TOKS, dim), F32)
            dg = jnp.zeros((TOKS, 8), F32)
            for e in range(EXPERTS):
                od = slots.spread(e, b, od_all.at[e], ALIGN)
                dx += od[:, dim:]
                dg += jnp.where(lane == slots.choice(e, b), jnp.sum(dy * od[:, :dim], axis=1, keepdims=True), 0.0)
            dx_buf[i, toks, :] = dx
            dx_buf[i, tok : tok + 8, toks] = dg.T
        copies.append(pltpu.make_async_copy(dx_buf.at[i], ref, dx_sems.at[i]))
        copies[-1].start()
    for copy in copies:
        copy.wait()


def dw_kernel(starts_ref, kept_hbm, dw1_hbm, dw3_hbm, dw2_hbm, kept, dw1, dw3, dw2, k_sems, o_sems):
    dim, width = dw1.shape[1:]
    slots = Slots(starts_ref, None, None, kept_hbm.shape[1] // TOKS)

    def copy_in(e, k, slot):
        rows = pl.ds(pl.multiple_of(k * 2 * ROWS, 2 * ROWS), 2 * ROWS)
        return pltpu.make_async_copy(kept_hbm.at[e, rows, :], kept.at[slot], k_sems.at[slot])

    def copy_out(e, i):
        return pltpu.make_async_copy((dw1, dw3, dw2)[i].at[e], (dw1_hbm, dw3_hbm, dw2_hbm)[i].at[e], o_sems.at[e, i])

    first_tiles = (slots.tiles(0) + 1) // 2
    count = first_tiles + (slots.tiles(1) + 1) // 2

    def where(g):
        e = (g >= first_tiles).astype(jnp.int32)
        return e, g - e * first_tiles

    copy_in(*where(0), 0).start()

    def tile(g, carry):
        slot = lax.rem(g, 2)
        e, k = where(g)
        copy_in(e, k, slot).wait()

        @pl.when(g + 1 < count)
        def _():
            copy_in(*where(g + 1), 1 - slot).start()

        @pl.when(2 * k + 1 == slots.tiles(e))
        def _():
            kept[slot, ROWS:, :] = jnp.zeros((ROWS, kept.shape[2]), BF)

        u = kept[slot, :, 3 * width : 3 * width + dim]
        q = kept[slot, :, 3 * width + dim :]
        fresh = k == 0
        last = (g == first_tiles - 1) | (g == count - 1)

        def put(ref, index, part):
            ref[index] = jnp.where(fresh, part, ref[index] + part)

        def leave(i):
            pl.when(last)(lambda: copy_out(e, i).start())

        for c in range(0, width, COLS):
            put(dw1, (e, slice(None), slice(c, c + COLS)), mm_tn(u, kept[slot, :, width + c : width + c + COLS]))
        leave(0)
        for c in range(0, width, COLS):
            put(dw3, (e, slice(None), slice(c, c + COLS)), mm_tn(u, kept[slot, :, 2 * width + c : 2 * width + c + COLS]))
        leave(1)
        for c in range(0, width, COLS):
            put(dw2, (e, slice(c, c + COLS), slice(None)), mm_tn(kept[slot, :, c : c + COLS], q))
        leave(2)
        return carry

    lax.fori_loop(0, count, tile, 0)
    for e in range(EXPERTS):
        for i in range(3):
            copy_out(e, i).wait()


IN_VMEM = pl.BlockSpec(memory_space=pltpu.VMEM)
IN_SMEM = pl.BlockSpec(memory_space=pltpu.SMEM)
IN_HBM = pl.BlockSpec(memory_space=pl.ANY)


def call(kernel, operands, in_specs, outs, out_specs, scratch, flops):
    return pl.pallas_call(
        kernel,
        in_specs=in_specs,
        out_specs=out_specs,
        out_shape=outs,
        scratch_shapes=scratch,
        compiler_params=pltpu.CompilerParams(vmem_limit_bytes=VMEM),
        cost_estimate=pl.CostEstimate(flops=flops, bytes_accessed=40_000_000, transcendentals=0),
    )(*operands)


def run_gather(own_map, x):
    tok, dim = x.shape
    tokens = 4 * tok
    pieces = 4
    outs = []
    for size in (tokens, tokens, tokens // 2, tokens // 2):
        outs.append(jax.ShapeDtypeStruct((EXPERTS, 128), jnp.int32))
        outs.append(jax.ShapeDtypeStruct((EXPERTS, size), F32))
        outs.append(jax.ShapeDtypeStruct((size, 8), F32))
    dma = pltpu.SemaphoreType.DMA
    out = pl.pallas_call(
        gather_kernel,
        in_specs=[IN_VMEM] * 2,
        out_specs=[IN_HBM] * 3 + [IN_VMEM] * 12,
        out_shape=[jax.ShapeDtypeStruct((tok, dim), BF)] * 3 + outs,
        scratch_shapes=[pltpu.VMEM((3, *own_map.shape), F32), pltpu.VMEM((3, tok, dim), BF)]
        + [dma((3,)), dma((3,))] + [dma((pieces,))] * 4 + [dma, dma, dma((2 * pieces + 1,))],
        compiler_params=pltpu.CompilerParams(collective_id=0, has_side_effects=True, vmem_limit_bytes=VMEM),
        cost_estimate=pl.CostEstimate(flops=10_000_000, bytes_accessed=4_000_000, transcendentals=0),
        name="gather_slots",
    )(own_map, x)
    maps = out[3:]
    return (out[0], out[1], x, out[2]), (maps[0:3], maps[3:6], maps[6:9], maps[9:12])


def weight_scratch(w1, w2):
    return [pltpu.VMEM(w1.shape, BF), pltpu.VMEM(w1.shape, BF), pltpu.VMEM(w2.shape, BF)]


def run_forward(xs, maps, w1, w3, w2):
    tok, dim = xs[0].shape
    tokens = tok * len(xs)
    width = w1.shape[2]
    most = tokens + TOKS + ALIGN + ROWS
    return call(
        functools.partial(forward_kernel, len(xs)), (maps[0], *xs, maps[1], maps[2], w1, w3, w2),
        [IN_SMEM] + [IN_VMEM] * (len(xs) + 2) + [IN_HBM] * 3,
        [jax.ShapeDtypeStruct((tok, dim), F32)] * len(xs),
        [IN_HBM] * len(xs),
        weight_scratch(w1, w2)
        + [pltpu.VMEM((EXPERTS, most, dim), BF)] * 2
        + [pltpu.VMEM((ROWS, width), BF), pltpu.VMEM((len(xs), tok, dim), F32)]
        + [pltpu.SemaphoreType.DMA((EXPERTS, 3)), pltpu.SemaphoreType.DMA((len(xs),))],
        2 * 3 * tokens * dim * width,
    )


def run_dx(xs, gs, maps, w1, w3, w2):
    tok, dim = xs[0].shape
    tokens = tok * len(xs)
    width = w1.shape[2]
    most = tokens + TOKS + ALIGN + ROWS
    kept = 3 * width + 2 * dim
    out = call(
        dx_kernel, (maps[0], *xs, *gs, maps[1], maps[2], w1, w3, w2),
        [IN_SMEM] + [IN_VMEM] * 10 + [IN_HBM] * 3,
        [jax.ShapeDtypeStruct((tok + 8, dim), F32)] * 4 + [jax.ShapeDtypeStruct((EXPERTS, tokens, kept), BF)],
        [IN_HBM] * 5,
        weight_scratch(w1, w2)
        + [pltpu.VMEM((EXPERTS, most, dim), BF)] * 2
        + [pltpu.VMEM((EXPERTS, most, 2 * dim), BF), pltpu.VMEM((2, ROWS, kept), BF), pltpu.VMEM((4, tok + 8, dim), F32)]
        + [pltpu.SemaphoreType.DMA((EXPERTS, 3)), pltpu.SemaphoreType.DMA((2,)), pltpu.SemaphoreType.DMA((4,))],
        2 * 6 * tokens * dim * width,
    )
    return out[:4], out[4]


def run_dw(kept, maps, shape1, shape2):
    tokens = kept.shape[1]
    return call(
        dw_kernel, (maps[0], kept),
        [IN_SMEM, IN_HBM],
        [jax.ShapeDtypeStruct(shape1, F32), jax.ShapeDtypeStruct(shape1, F32), jax.ShapeDtypeStruct(shape2, F32)],
        [IN_HBM] * 3,
        [pltpu.VMEM((2, 2 * ROWS, kept.shape[2]), BF), pltpu.VMEM(shape1, F32), pltpu.VMEM(shape1, F32), pltpu.VMEM(shape2, F32)]
        + [pltpu.SemaphoreType.DMA((2,)), pltpu.SemaphoreType.DMA((EXPERTS, 3))],
        2 * 3 * tokens * shape1[1] * shape1[2],
    )


def solution(mesh):
    tok_spec = P(("dp", "ep"))
    w_spec = P("ep")
    across = [(0, 2), (2, 0), (1, 3), (3, 1)]
    beside = [(0, 1), (1, 0), (2, 3), (3, 2)]
    cross = [(0, 3), (3, 0), (1, 2), (2, 1)]

    def permute(v, pairs):
        return lax.ppermute(v, "ep", pairs)

    def gather(own):
        other = permute(own, across)
        return other, permute(other, beside), own, permute(own, beside)

    def gather_direct(own):
        return permute(own, across), permute(own, cross), own, permute(own, beside)

    def combine(parts):
        other, diagonal, own, mate = parts
        theirs = other + permute(diagonal, beside)
        return own + permute(mate, beside) + permute(theirs, across)

    def device_program(x_in, idx_a, idx_b, gate_a, gate_b, dy_out, w1_a, w3_a, w2_a, w1_b, w3_b, w2_b):
        tok, top_k = idx_a.shape
        own_map = jnp.concatenate([idx_a.astype(F32), idx_b.astype(F32), gate_a, gate_b], axis=1).T
        x_all, (maps_a, maps_b, maps_far, maps_near) = run_gather(own_map, x_in)

        def add(base, total):
            return (base.astype(F32) + total[:tok]).astype(BF)

        def dgate_of(total):
            return total[tok : tok + top_k].T

        dy_own, x_other = lax.optimization_barrier((dy_out, x_all[0]))
        x_all = (x_other, *x_all[1:])
        dy_all = gather(dy_own)
        far_parts = run_forward(x_all[:2], maps_far, w1_a, w3_a, w2_a)
        near_parts = run_forward(x_all[2:], maps_near, w1_a, w3_a, w2_a)
        x_mid = add(x_in, combine((*far_parts, *near_parts)))
        mid_all = gather(x_mid)
        x_again, mid_other = lax.optimization_barrier((x_in, mid_all[0]))
        mid_all = (mid_other, *mid_all[1:])
        again_all = gather_direct(x_again)
        dx_parts, kept_b = run_dx(mid_all, dy_all, maps_b, w1_b, w3_b, w2_b)
        total = combine(dx_parts)
        dx_mid, dgate_b = add(dy_out, total), dgate_of(total)
        dmid_all = gather_direct(dx_mid)
        x_out = add(x_mid, combine(run_forward(mid_all, maps_b, w1_b, w3_b, w2_b)))
        grads_b = run_dw(kept_b, maps_b, w1_b.shape, w2_b.shape)
        dx_parts, kept_a = run_dx(again_all, dmid_all, maps_a, w1_a, w3_a, w2_a)
        total = combine(dx_parts)
        dx_in, dgate_a = add(dx_mid, total), dgate_of(total)
        grads_a = run_dw(kept_a, maps_a, w1_a.shape, w2_a.shape)
        return (x_out, dx_in, *grads_a, *grads_b, dgate_a, dgate_b)


    return jax.shard_map(device_program, mesh=mesh, in_specs=(tok_spec,) * 6 + (w_spec,) * 6, out_specs=(tok_spec,) * 10, check_vma=False)
```

```python
import functools

import jax
import jax.numpy as jnp
from jax import lax
from jax.experimental import pallas as pl
from jax.experimental.pallas import tpu as pltpu
from jax.sharding import PartitionSpec as P


ROWS = 256
TOKS = 256
ALIGN = 16
COLS = 256
EXPERTS = 2
VMEM = 66_000_000

BF = jnp.bfloat16
F32 = jnp.float32


def mm(a, b):
    return lax.dot_general(a, b, (((1,), (0,)), ((), ())), preferred_element_type=F32)


def mm_nt(a, b):
    return lax.dot_general(a, b, (((1,), (1,)), ((), ())), preferred_element_type=F32)


def mm_tn(a, b):
    return lax.dot_general(a, b, (((0,), (0,)), ((), ())), preferred_element_type=F32)


def block_of(refs, b):
    per = refs[0].shape[0] // TOKS
    return refs[b // per], slice((b % per) * TOKS, (b % per + 1) * TOKS)


def tile_rows(k):
    return pl.ds(pl.multiple_of(k * ROWS, ROWS), ROWS)


class Slots:
    def __init__(self, starts_ref, rows_ref, cols_ref, blocks):
        self.starts_ref, self.rows_ref, self.cols_ref, self.blocks = starts_ref, rows_ref, cols_ref, blocks

    def tiles(self, e):
        return (self.starts_ref[e, self.blocks] + ROWS - 1) // ROWS

    def rows(self, e, b):
        return pl.ds(pl.multiple_of(self.starts_ref[e, b], ALIGN), TOKS)

    def base(self, e, b):
        return self.starts_ref[e, b].astype(F32)

    def col(self, b, i):
        rows = slice(b * TOKS, (b + 1) * TOKS) if isinstance(b, int) else pl.ds(pl.multiple_of(b * TOKS, TOKS), TOKS)
        return self.cols_ref[rows, i : i + 1]

    def gate(self, e, b):
        if isinstance(e, int):
            return self.col(b, EXPERTS + e)
        return jnp.where(e == 0, self.col(b, EXPERTS), self.col(b, EXPERTS + 1))

    def choice(self, e, b):
        return self.col(b, 2 * EXPERTS + e)

    def compact(self, e, makers, outs):
        line = lax.broadcasted_iota(jnp.int32, (TOKS, TOKS), 0).astype(F32)
        for b in range(self.blocks):
            slot = self.rows_ref[pl.ds(e, 1), b * TOKS : (b + 1) * TOKS] - self.base(e, b)
            hot = jnp.where(slot == line, 1.0, 0.0).astype(BF)
            for make, out in zip(makers, outs):
                out[self.rows(e, b), :] = mm(hot, make(b)).astype(BF)
        end = pl.multiple_of(self.starts_ref[e, self.blocks - 1] + TOKS, ALIGN)
        for out in outs:
            out[pl.ds(end, ROWS), :] = jnp.zeros((ROWS, out.shape[1]), BF)

    def spread(self, e, b, ref, more=0):
        line = lax.broadcasted_iota(jnp.int32, (TOKS, TOKS + more), 1).astype(F32)
        hot = jnp.where(self.col(b, e) - self.base(e, b) == line, 1.0, 0.0).astype(BF)
        rows = pl.ds(pl.multiple_of(self.starts_ref[e, b], ALIGN), TOKS + more)
        return mm(hot, ref[rows, :])

    def zero_after(self, e, ref):
        end = pl.multiple_of(self.tiles(e) * ROWS, ROWS)
        ref[pl.ds(end, TOKS + ALIGN), :] = jnp.zeros((TOKS + ALIGN, ref.shape[1]), BF)


def find_slots(tables, refs):
    full_a, full_b, halves = refs[0:3], refs[3:6], (refs[6:9], refs[9:12])
    tok = tables[0].shape[1]
    blocks = len(tables) * tok // TOKS
    half = blocks // 2
    first = (lax.axis_index("ep") * EXPERTS).astype(F32)
    line = lax.broadcasted_iota(jnp.int32, (8, TOKS), 0)
    target = first + (line % EXPERTS).astype(F32)
    lane = lax.broadcasted_iota(jnp.int32, (8, 128), 1)
    upto = (lax.broadcasted_iota(jnp.int32, (TOKS, TOKS), 0) <= lax.broadcasted_iota(jnp.int32, (TOKS, TOKS), 1)).astype(F32).astype(BF)
    seen = jnp.zeros((8, 1), F32)
    before = jnp.zeros((8, 1), F32)
    starts = jnp.zeros((8, 128), F32)
    later = jnp.zeros((8, 128), F32)
    for b in range(blocks):
        at = b * TOKS
        table = tables[at // tok][:, at % tok : at % tok + TOKS]
        if b == half:
            before = seen

        def both(i, other):
            return jnp.where(line < EXPERTS, table[i : i + 1], jnp.where(line < 2 * EXPERTS, table[i + 2 : i + 3], other))

        hit0 = both(0, -1.0) == target
        hit1 = both(1, -1.0) == target
        mask = jnp.where(hit0 | hit1, 1.0, 0.0)
        count = mm(mask.astype(BF), upto)
        slot = jnp.where(mask > 0.0, seen + count - 1.0, -1.0)
        part_slot = jnp.where(mask > 0.0, seen - before + count - 1.0, -1.0)
        gate = jnp.where(hit0, both(4, 0.0), 0.0) + jnp.where(hit1, both(5, 0.0), 0.0)
        choice = jnp.where(hit1, 1.0, 0.0)
        starts = jnp.where(lane == b, seen, starts)
        if b >= half:
            later = jnp.where(lane == b - half, seen - before, later)

        def put(outs, layer, here, slots):
            part = slice(layer * EXPERTS, (layer + 1) * EXPERTS)
            outs[1][:, here : here + TOKS] = slots[part]
            stack = jnp.concatenate([slots[part], gate[part], choice[part], choice[part]], axis=0)
            outs[2][here : here + TOKS, :] = stack.T

        put(full_a, 0, at, slot)
        put(full_b, 1, at, slot)
        put(halves[b // half], 0, at % (half * TOKS), part_slot)
        seen = seen + jnp.floor((count[:, TOKS - 1 :] + (ALIGN - 1.0)) / ALIGN) * ALIGN
    starts = jnp.where(lane == blocks, seen, starts).astype(jnp.int32)
    later = jnp.where(lane == half, seen - before, later).astype(jnp.int32)
    full_a[0][...] = starts[:EXPERTS]
    full_b[0][...] = starts[EXPERTS : 2 * EXPERTS]
    halves[0][0][...] = starts[:EXPERTS]
    halves[1][0][...] = later[:EXPERTS]


def gather_kernel(map_ref, x_ref, other_hbm, diagonal_hbm, mate_hbm, *refs):
    slot_hbm, slot_refs = refs[:12], refs[12:24]
    maps, held, map_send, map_recv, far_send, far_recv, hop_send, hop_recv, near_send, near_recv, out_sems, slot_sems = refs[24:]
    me = lax.axis_index("ep")
    mate = me + 1 - 2 * lax.rem(me, 2)
    other = lax.rem(me + 2, 4)
    diagonal = lax.rem(mate + 2, 4)
    pieces = far_send.shape[0]
    size = x_ref.shape[0] // pieces

    def send(src, dst, send_sem, recv_sem, to):
        return pltpu.make_async_remote_copy(
            src_ref=src, dst_ref=dst, send_sem=send_sem, recv_sem=recv_sem,
            device_id={"ep": to}, device_id_type=pl.DeviceIdType.MESH,
        )

    barrier = pltpu.get_barrier_semaphore()
    for peer in (other, diagonal, mate):
        pl.semaphore_signal(barrier, inc=1, device_id={"ep": peer}, device_id_type=pl.DeviceIdType.MESH)
    pl.semaphore_wait(barrier, 3)

    map_copies = [send(map_ref, maps.at[i], map_send.at[i], map_recv.at[i], to) for i, to in enumerate((other, diagonal, mate))]
    for copy in map_copies:
        copy.start()
    part = [pl.ds(p * size, size) for p in range(pieces)]
    far = [send(x_ref.at[part[p], :], held.at[0, part[p], :], far_send.at[p], far_recv.at[p], other) for p in range(pieces)]
    for copy in far:
        copy.start()
    near = send(x_ref, held.at[2], near_send, near_recv, mate)
    near.start()
    for copy in map_copies:
        copy.wait_recv()
    find_slots((maps.at[0], maps.at[1], map_ref, maps.at[2]), slot_refs)
    slot_copies = [pltpu.make_async_copy(v, h, slot_sems.at[i]) for i, (v, h) in enumerate(zip(slot_refs, slot_hbm))]
    for copy in slot_copies:
        copy.start()
    near.wait()
    outs = [pltpu.make_async_copy(held.at[2], mate_hbm, out_sems.at[2 * pieces])]
    outs[0].start()
    hops = []
    for p in range(pieces):
        far[p].wait_recv()
        hops.append(send(held.at[0, part[p], :], held.at[1, part[p], :], hop_send.at[p], hop_recv.at[p], mate))
        hops[p].start()
        outs.append(pltpu.make_async_copy(held.at[0, part[p], :], other_hbm.at[part[p], :], out_sems.at[p]))
        outs[-1].start()
    for p in range(pieces):
        hops[p].wait_recv()
        outs.append(pltpu.make_async_copy(held.at[1, part[p], :], diagonal_hbm.at[part[p], :], out_sems.at[pieces + p]))
        outs[-1].start()
    for copy in map_copies + far + hops:
        copy.wait_send()
    for copy in outs + slot_copies:
        copy.wait()


def weight_copies(hbm, vmem, sems, e):
    return [pltpu.make_async_copy(h.at[e], v.at[e], sems.at[e, i]) for i, (h, v) in enumerate(zip(hbm, vmem))]


def forward_kernel(n, starts_ref, *refs):
    xs, (rows_ref, cols_ref, w1_hbm, w3_hbm, w2_hbm), ys = refs[:n], refs[n : n + 5], refs[n + 5 : 2 * n + 5]
    w1, w3, w2, u_all, o_all, h_ref, y_buf, w_sems, y_sems = refs[2 * n + 5 :]
    blocks = rows_ref.shape[1] // TOKS
    width = w1.shape[2]
    slots = Slots(starts_ref, rows_ref, cols_ref, blocks)
    for e in range(EXPERTS):
        for copy in weight_copies((w1_hbm, w3_hbm, w2_hbm), (w1, w3, w2), w_sems, e):
            copy.start()

    def tokens_of(b):
        ref, toks = block_of(xs, b)
        return ref[toks, :]

    def gather_rows(e, carry):
        slots.compact(e, (tokens_of,), (u_all.at[e],))
        return carry

    lax.fori_loop(0, EXPERTS, gather_rows, 0)

    def expert(e, carry):
        for copy in weight_copies((w1_hbm, w3_hbm, w2_hbm), (w1, w3, w2), w_sems, e):
            copy.wait()

        def tile(k, inner):
            u = u_all[e, tile_rows(k), :]
            for c in range(0, width, COLS):
                cols = slice(c, c + COLS)
                a = mm(u, w1[e, :, cols])
                b = mm(u, w3[e, :, cols])
                h_ref[:, cols] = (a * jax.nn.sigmoid(a) * b).astype(BF)
            o_all[e, tile_rows(k), :] = mm(h_ref[...], w2[e]).astype(BF)
            return inner

        return lax.fori_loop(0, slots.tiles(e), tile, carry)

    lax.fori_loop(0, EXPERTS, expert, 0)
    for e in range(EXPERTS):
        slots.zero_after(e, o_all.at[e])
    each = ys[0].shape[0] // TOKS

    def send_home(i, carry):
        for j in range(each):
            b = i * each + j
            toks = slice(j * TOKS, (j + 1) * TOKS)
            y_buf[i, toks, :] = sum(slots.gate(e, b) * slots.spread(e, b, o_all.at[e]) for e in range(EXPERTS))
        for n, ref in enumerate(ys):
            pl.when(i == n)(lambda: pltpu.make_async_copy(y_buf.at[n], ref, y_sems.at[n]).start())
        return carry

    lax.fori_loop(0, len(ys), send_home, 0)
    for n, ref in enumerate(ys):
        pltpu.make_async_copy(y_buf.at[n], ref, y_sems.at[n]).wait()


def dx_kernel(starts_ref, x0, x1, x2, x3, g0, g1, g2, g3, rows_ref, cols_ref, w1_hbm, w3_hbm, w2_hbm,
              dx0, dx1, dx2, dx3, kept_hbm, w1, w3, w2, u_all, q_all, od_all, kept, dx_buf, w_sems, k_sems, dx_sems):
    xs, gs, dxs = (x0, x1, x2, x3), (g0, g1, g2, g3), (dx0, dx1, dx2, dx3)
    tok = x0.shape[0]
    blocks = rows_ref.shape[1] // TOKS
    dim, width = w1.shape[1:]
    slots = Slots(starts_ref, rows_ref, cols_ref, blocks)
    for e in range(EXPERTS):
        for copy in weight_copies((w1_hbm, w3_hbm, w2_hbm), (w1, w3, w2), w_sems, e):
            copy.start()

    def tokens_of(b):
        ref, toks = block_of(xs, b)
        return ref[toks, :]

    def gather_rows(e, carry):
        def scaled_of(b):
            ref, toks = block_of(gs, b)
            return (slots.gate(e, b) * ref[toks, :].astype(F32)).astype(BF)

        slots.compact(e, (tokens_of, scaled_of), (u_all.at[e], q_all.at[e]))
        return carry

    lax.fori_loop(0, EXPERTS, gather_rows, 0)

    def copy_out(e, k):
        return pltpu.make_async_copy(kept.at[lax.rem(k, 2)], kept_hbm.at[e, tile_rows(k), :], k_sems.at[lax.rem(k, 2)])

    def expert(e, carry):
        for copy in weight_copies((w1_hbm, w3_hbm, w2_hbm), (w1, w3, w2), w_sems, e):
            copy.wait()
        count = slots.tiles(e)

        def tile(k, inner):
            slot = lax.rem(k, 2)

            @pl.when(k >= 2)
            def _():
                copy_out(e, k - 2).wait()

            u = u_all[e, tile_rows(k), :]
            q = q_all[e, tile_rows(k), :]
            for c in range(0, width, COLS):
                cols = slice(c, c + COLS)
                a = mm(u, w1[e, :, cols])
                b = mm(u, w3[e, :, cols])
                dh = mm_nt(q, w2[e, cols, :])
                s = jax.nn.sigmoid(a)
                act = a * s
                kept[slot, :, c : c + COLS] = (act * b).astype(BF)
                kept[slot, :, width + c : width + c + COLS] = (dh * b * s * (1.0 + a * (1.0 - s))).astype(BF)
                kept[slot, :, 2 * width + c : 2 * width + c + COLS] = (dh * act).astype(BF)
            kept[slot, :, 3 * width : 3 * width + dim] = u
            kept[slot, :, 3 * width + dim :] = q
            od_all[e, tile_rows(k), :dim] = mm(kept[slot, :, :width], w2[e]).astype(BF)
            du = mm_nt(kept[slot, :, width : 2 * width], w1[e]) + mm_nt(kept[slot, :, 2 * width : 3 * width], w3[e])
            od_all[e, tile_rows(k), dim:] = du.astype(BF)
            copy_out(e, k).start()
            return inner

        lax.fori_loop(0, count, tile, 0)

        @pl.when(count >= 2)
        def _():
            copy_out(e, count - 2).wait()

        @pl.when(count >= 1)
        def _():
            copy_out(e, count - 1).wait()

        return carry

    lax.fori_loop(0, EXPERTS, expert, 0)
    for e in range(EXPERTS):
        slots.zero_after(e, od_all.at[e])
    copies = []
    each = tok // TOKS
    lane = lax.broadcasted_iota(jnp.int32, (TOKS, 8), 1).astype(F32)
    for i, ref in enumerate(dxs):

        for j in range(each):
            b = i * each + j
            toks = slice(j * TOKS, (j + 1) * TOKS)
            dy = gs[i][toks, :].astype(F32)
            dx = jnp.zeros((TOKS, dim), F32)
            dg = jnp.zeros((TOKS, 8), F32)
            for e in range(EXPERTS):
                od = slots.spread(e, b, od_all.at[e], ALIGN)
                dx += od[:, dim:]
                dg += jnp.where(lane == slots.choice(e, b), jnp.sum(dy * od[:, :dim], axis=1, keepdims=True), 0.0)
            dx_buf[i, toks, :] = dx
            dx_buf[i, tok : tok + 8, toks] = dg.T
        copies.append(pltpu.make_async_copy(dx_buf.at[i], ref, dx_sems.at[i]))
        copies[-1].start()
    for copy in copies:
        copy.wait()


def dw_kernel(starts_ref, kept_hbm, dw1_hbm, dw3_hbm, dw2_hbm, kept, dw1, dw3, dw2, k_sems, o_sems):
    dim, width = dw1.shape[1:]
    slots = Slots(starts_ref, None, None, kept_hbm.shape[1] // TOKS)

    def copy_in(e, k, slot):
        rows = pl.ds(pl.multiple_of(k * 2 * ROWS, 2 * ROWS), 2 * ROWS)
        return pltpu.make_async_copy(kept_hbm.at[e, rows, :], kept.at[slot], k_sems.at[slot])

    def copy_out(e, i):
        return pltpu.make_async_copy((dw1, dw3, dw2)[i].at[e], (dw1_hbm, dw3_hbm, dw2_hbm)[i].at[e], o_sems.at[e, i])

    first = (slots.tiles(1) > slots.tiles(0)).astype(jnp.int32)
    first_tiles = (slots.tiles(first) + 1) // 2
    count = first_tiles + (slots.tiles(1 - first) + 1) // 2

    def where(g):
        second = (g >= first_tiles).astype(jnp.int32)
        return jnp.where(second == 0, first, 1 - first), g - second * first_tiles

    copy_in(*where(0), 0).start()

    def tile(g, carry):
        slot = lax.rem(g, 2)
        e, k = where(g)
        copy_in(e, k, slot).wait()

        @pl.when(g + 1 < count)
        def _():
            copy_in(*where(g + 1), 1 - slot).start()

        @pl.when(2 * k + 1 == slots.tiles(e))
        def _():
            kept[slot, ROWS:, :] = jnp.zeros((ROWS, kept.shape[2]), BF)

        u = kept[slot, :, 3 * width : 3 * width + dim]
        q = kept[slot, :, 3 * width + dim :]
        fresh = k == 0
        last = (g == first_tiles - 1) | (g == count - 1)

        def put(ref, index, part):
            ref[index] = jnp.where(fresh, part, ref[index] + part)

        def leave(i):
            pl.when(last)(lambda: copy_out(e, i).start())

        for c in range(0, width, COLS):
            put(dw1, (e, slice(None), slice(c, c + COLS)), mm_tn(u, kept[slot, :, width + c : width + c + COLS]))
        leave(0)
        for c in range(0, width, COLS):
            put(dw3, (e, slice(None), slice(c, c + COLS)), mm_tn(u, kept[slot, :, 2 * width + c : 2 * width + c + COLS]))
        leave(1)
        for c in range(0, width, COLS):
            put(dw2, (e, slice(c, c + COLS), slice(None)), mm_tn(kept[slot, :, c : c + COLS], q))
        leave(2)
        return carry

    lax.fori_loop(0, count, tile, 0)
    for e in range(EXPERTS):
        for i in range(3):
            copy_out(e, i).wait()


IN_VMEM = pl.BlockSpec(memory_space=pltpu.VMEM)
IN_SMEM = pl.BlockSpec(memory_space=pltpu.SMEM)
IN_HBM = pl.BlockSpec(memory_space=pl.ANY)


def call(kernel, operands, in_specs, outs, out_specs, scratch, flops):
    return pl.pallas_call(
        kernel,
        in_specs=in_specs,
        out_specs=out_specs,
        out_shape=outs,
        scratch_shapes=scratch,
        compiler_params=pltpu.CompilerParams(vmem_limit_bytes=VMEM),
        cost_estimate=pl.CostEstimate(flops=flops, bytes_accessed=40_000_000, transcendentals=0),
    )(*operands)


def run_gather(own_map, x):
    tok, dim = x.shape
    tokens = 4 * tok
    pieces = 4
    outs = []
    for size in (tokens, tokens, tokens // 2, tokens // 2):
        outs.append(jax.ShapeDtypeStruct((EXPERTS, 128), jnp.int32))
        outs.append(jax.ShapeDtypeStruct((EXPERTS, size), F32))
        outs.append(jax.ShapeDtypeStruct((size, 8), F32))
    dma = pltpu.SemaphoreType.DMA
    out = pl.pallas_call(
        gather_kernel,
        in_specs=[IN_VMEM] * 2,
        out_specs=[IN_HBM] * 15,
        out_shape=[jax.ShapeDtypeStruct((tok, dim), BF)] * 3 + outs,
        scratch_shapes=[pltpu.VMEM(out.shape, out.dtype) for out in outs]
        + [pltpu.VMEM((3, *own_map.shape), F32), pltpu.VMEM((3, tok, dim), BF)]
        + [dma((3,)), dma((3,))] + [dma((pieces,))] * 4 + [dma, dma, dma((2 * pieces + 1,)), dma((12,))],
        compiler_params=pltpu.CompilerParams(collective_id=0, has_side_effects=True, vmem_limit_bytes=VMEM),
        cost_estimate=pl.CostEstimate(flops=10_000_000, bytes_accessed=4_000_000, transcendentals=0),
        name="gather_slots",
    )(own_map, x)
    maps = out[3:]
    return (out[0], out[1], x, out[2]), (maps[0:3], maps[3:6], maps[6:9], maps[9:12])


def weight_scratch(w1, w2):
    return [pltpu.VMEM(w1.shape, BF), pltpu.VMEM(w1.shape, BF), pltpu.VMEM(w2.shape, BF)]


def run_forward(xs, maps, w1, w3, w2):
    tok, dim = xs[0].shape
    tokens = tok * len(xs)
    width = w1.shape[2]
    most = tokens + TOKS + ALIGN + ROWS
    return call(
        functools.partial(forward_kernel, len(xs)), (maps[0], *xs, maps[1], maps[2], w1, w3, w2),
        [IN_SMEM] + [IN_VMEM] * (len(xs) + 2) + [IN_HBM] * 3,
        [jax.ShapeDtypeStruct((tok, dim), F32)] * len(xs),
        [IN_HBM] * len(xs),
        weight_scratch(w1, w2)
        + [pltpu.VMEM((EXPERTS, most, dim), BF)] * 2
        + [pltpu.VMEM((ROWS, width), BF), pltpu.VMEM((len(xs), tok, dim), F32)]
        + [pltpu.SemaphoreType.DMA((EXPERTS, 3)), pltpu.SemaphoreType.DMA((len(xs),))],
        2 * 3 * tokens * dim * width,
    )


def run_dx(xs, gs, maps, w1, w3, w2):
    tok, dim = xs[0].shape
    tokens = tok * len(xs)
    width = w1.shape[2]
    most = tokens + TOKS + ALIGN + ROWS
    kept = 3 * width + 2 * dim
    out = call(
        dx_kernel, (maps[0], *xs, *gs, maps[1], maps[2], w1, w3, w2),
        [IN_SMEM] + [IN_VMEM] * 10 + [IN_HBM] * 3,
        [jax.ShapeDtypeStruct((tok + 8, dim), F32)] * 4 + [jax.ShapeDtypeStruct((EXPERTS, tokens, kept), BF)],
        [IN_HBM] * 5,
        weight_scratch(w1, w2)
        + [pltpu.VMEM((EXPERTS, most, dim), BF)] * 2
        + [pltpu.VMEM((EXPERTS, most, 2 * dim), BF), pltpu.VMEM((2, ROWS, kept), BF), pltpu.VMEM((4, tok + 8, dim), F32)]
        + [pltpu.SemaphoreType.DMA((EXPERTS, 3)), pltpu.SemaphoreType.DMA((2,)), pltpu.SemaphoreType.DMA((4,))],
        2 * 6 * tokens * dim * width,
    )
    return out[:4], out[4]


def run_dw(kept, maps, shape1, shape2):
    tokens = kept.shape[1]
    return call(
        dw_kernel, (maps[0], kept),
        [IN_SMEM, IN_HBM],
        [jax.ShapeDtypeStruct(shape1, F32), jax.ShapeDtypeStruct(shape1, F32), jax.ShapeDtypeStruct(shape2, F32)],
        [IN_HBM] * 3,
        [pltpu.VMEM((2, 2 * ROWS, kept.shape[2]), BF), pltpu.VMEM(shape1, F32), pltpu.VMEM(shape1, F32), pltpu.VMEM(shape2, F32)]
        + [pltpu.SemaphoreType.DMA((2,)), pltpu.SemaphoreType.DMA((EXPERTS, 3))],
        2 * 3 * tokens * shape1[1] * shape1[2],
    )


def solution(mesh):
    tok_spec = P(("dp", "ep"))
    w_spec = P("ep")
    across = [(0, 2), (2, 0), (1, 3), (3, 1)]
    beside = [(0, 1), (1, 0), (2, 3), (3, 2)]
    cross = [(0, 3), (3, 0), (1, 2), (2, 1)]

    def permute(v, pairs):
        return lax.ppermute(v, "ep", pairs)

    def gather(own):
        other = permute(own, across)
        return other, permute(other, beside), own, permute(own, beside)

    def gather_direct(own):
        return permute(own, across), permute(own, cross), own, permute(own, beside)

    def combine(parts):
        other, diagonal, own, mate = parts
        theirs = other + permute(diagonal, beside)
        return own + permute(mate, beside) + permute(theirs, across)

    def device_program(x_in, idx_a, idx_b, gate_a, gate_b, dy_out, w1_a, w3_a, w2_a, w1_b, w3_b, w2_b):
        tok, top_k = idx_a.shape
        own_map = jnp.concatenate([idx_a.astype(F32), idx_b.astype(F32), gate_a, gate_b], axis=1).T
        x_all, (maps_a, maps_b, maps_far, maps_near) = run_gather(own_map, x_in)

        def add(base, total):
            return (base.astype(F32) + total[:tok]).astype(BF)

        def dgate_of(total):
            return total[tok : tok + top_k].T

        dy_own, x_other = lax.optimization_barrier((dy_out, x_all[0]))
        x_all = (x_other, *x_all[1:])
        dy_all = gather(dy_own)
        far_parts = run_forward(x_all[:2], maps_far, w1_a, w3_a, w2_a)
        near_parts = run_forward(x_all[2:], maps_near, w1_a, w3_a, w2_a)
        x_mid = add(x_in, combine((*far_parts, *near_parts)))
        mid_all = gather(x_mid)
        x_again, mid_other = lax.optimization_barrier((x_in, mid_all[0]))
        mid_all = (mid_other, *mid_all[1:])
        again_all = gather_direct(x_again)
        dx_parts, kept_b = run_dx(mid_all, dy_all, maps_b, w1_b, w3_b, w2_b)
        total = combine(dx_parts)
        dx_mid, dgate_b = add(dy_out, total), dgate_of(total)
        dmid_all = gather_direct(dx_mid)
        x_out = add(x_mid, combine(run_forward(mid_all, maps_b, w1_b, w3_b, w2_b)))
        grads_b = run_dw(kept_b, maps_b, w1_b.shape, w2_b.shape)
        dx_parts, kept_a = run_dx(again_all, dmid_all, maps_a, w1_a, w3_a, w2_a)
        total = combine(dx_parts)
        dx_in, dgate_a = add(dx_mid, total), dgate_of(total)
        grads_a = run_dw(kept_a, maps_a, w1_a.shape, w2_a.shape)
        return (x_out, dx_in, *grads_a, *grads_b, dgate_a, dgate_b)


    return jax.shard_map(device_program, mesh=mesh, in_specs=(tok_spec,) * 6 + (w_spec,) * 6, out_specs=(tok_spec,) * 10, check_vma=False)
```

```python
import functools

import jax
import jax.numpy as jnp
from jax import lax
from jax.experimental import pallas as pl
from jax.experimental.pallas import tpu as pltpu
from jax.sharding import PartitionSpec as P


ROWS = 256
TOKS = 256
ALIGN = 16
COLS = 256
EXPERTS = 2
VMEM = 66_000_000

BF = jnp.bfloat16
F32 = jnp.float32


def mm(a, b):
    return lax.dot_general(a, b, (((1,), (0,)), ((), ())), preferred_element_type=F32)


def mm_nt(a, b):
    return lax.dot_general(a, b, (((1,), (1,)), ((), ())), preferred_element_type=F32)


def mm_tn(a, b):
    return lax.dot_general(a, b, (((0,), (0,)), ((), ())), preferred_element_type=F32)


def block_of(refs, b):
    per = refs[0].shape[0] // TOKS
    return refs[b // per], slice((b % per) * TOKS, (b % per + 1) * TOKS)


def tile_rows(k):
    return pl.ds(pl.multiple_of(k * ROWS, ROWS), ROWS)


class Slots:
    def __init__(self, starts_ref, rows_ref, cols_ref, blocks):
        self.starts_ref, self.rows_ref, self.cols_ref, self.blocks = starts_ref, rows_ref, cols_ref, blocks

    def tiles(self, e):
        return (self.starts_ref[e, self.blocks] + ROWS - 1) // ROWS

    def rows(self, e, b):
        return pl.ds(pl.multiple_of(self.starts_ref[e, b], ALIGN), TOKS)

    def base(self, e, b):
        return self.starts_ref[e, b].astype(F32)

    def col(self, b, i):
        rows = slice(b * TOKS, (b + 1) * TOKS) if isinstance(b, int) else pl.ds(pl.multiple_of(b * TOKS, TOKS), TOKS)
        return self.cols_ref[rows, i : i + 1]

    def gate(self, e, b):
        if isinstance(e, int):
            return self.col(b, EXPERTS + e)
        return jnp.where(e == 0, self.col(b, EXPERTS), self.col(b, EXPERTS + 1))

    def choice(self, e, b):
        return self.col(b, 2 * EXPERTS + e)

    def compact(self, e, makers, outs):
        line = lax.broadcasted_iota(jnp.int32, (TOKS, TOKS), 0).astype(F32)
        for b in range(self.blocks):
            slot = self.rows_ref[pl.ds(e, 1), b * TOKS : (b + 1) * TOKS] - self.base(e, b)
            hot = jnp.where(slot == line, 1.0, 0.0).astype(BF)
            for make, out in zip(makers, outs):
                out[self.rows(e, b), :] = mm(hot, make(b)).astype(BF)
        end = pl.multiple_of(self.starts_ref[e, self.blocks - 1] + TOKS, ALIGN)
        for out in outs:
            out[pl.ds(end, ROWS), :] = jnp.zeros((ROWS, out.shape[1]), BF)

    def spread(self, e, b, ref, more=0):
        line = lax.broadcasted_iota(jnp.int32, (TOKS, TOKS + more), 1).astype(F32)
        hot = jnp.where(self.col(b, e) - self.base(e, b) == line, 1.0, 0.0).astype(BF)
        rows = pl.ds(pl.multiple_of(self.starts_ref[e, b], ALIGN), TOKS + more)
        return mm(hot, ref[rows, :])

    def zero_after(self, e, ref):
        end = pl.multiple_of(self.tiles(e) * ROWS, ROWS)
        ref[pl.ds(end, TOKS + ALIGN), :] = jnp.zeros((TOKS + ALIGN, ref.shape[1]), BF)


def find_slots(tables, refs):
    full_a, full_b, halves = refs[0:3], refs[3:6], (refs[6:9], refs[9:12])
    tok = tables[0].shape[1]
    blocks = len(tables) * tok // TOKS
    half = blocks // 2
    first = (lax.axis_index("ep") * EXPERTS).astype(F32)
    line = lax.broadcasted_iota(jnp.int32, (8, TOKS), 0)
    target = first + (line % EXPERTS).astype(F32)
    lane = lax.broadcasted_iota(jnp.int32, (8, 128), 1)
    upto = (lax.broadcasted_iota(jnp.int32, (TOKS, TOKS), 0) <= lax.broadcasted_iota(jnp.int32, (TOKS, TOKS), 1)).astype(F32).astype(BF)
    seen = jnp.zeros((8, 1), F32)
    before = jnp.zeros((8, 1), F32)
    starts = jnp.zeros((8, 128), F32)
    later = jnp.zeros((8, 128), F32)
    for b in range(blocks):
        at = b * TOKS
        table = tables[at // tok][:, at % tok : at % tok + TOKS]
        if b == half:
            before = seen

        def both(i, other):
            return jnp.where(line < EXPERTS, table[i : i + 1], jnp.where(line < 2 * EXPERTS, table[i + 2 : i + 3], other))

        hit0 = both(0, -1.0) == target
        hit1 = both(1, -1.0) == target
        mask = jnp.where(hit0 | hit1, 1.0, 0.0)
        count = mm(mask.astype(BF), upto)
        slot = jnp.where(mask > 0.0, seen + count - 1.0, -1.0)
        part_slot = jnp.where(mask > 0.0, seen - before + count - 1.0, -1.0)
        gate = jnp.where(hit0, both(4, 0.0), 0.0) + jnp.where(hit1, both(5, 0.0), 0.0)
        choice = jnp.where(hit1, 1.0, 0.0)
        starts = jnp.where(lane == b, seen, starts)
        if b >= half:
            later = jnp.where(lane == b - half, seen - before, later)

        def put(outs, layer, here, slots):
            part = slice(layer * EXPERTS, (layer + 1) * EXPERTS)
            outs[1][:, here : here + TOKS] = slots[part]
            stack = jnp.concatenate([slots[part], gate[part], choice[part], choice[part]], axis=0)
            outs[2][here : here + TOKS, :] = stack.T

        put(full_a, 0, at, slot)
        put(full_b, 1, at, slot)
        put(halves[b // half], 0, at % (half * TOKS), part_slot)
        seen = seen + jnp.floor((count[:, TOKS - 1 :] + (ALIGN - 1.0)) / ALIGN) * ALIGN
    starts = jnp.where(lane == blocks, seen, starts).astype(jnp.int32)
    later = jnp.where(lane == half, seen - before, later).astype(jnp.int32)
    full_a[0][...] = starts[:EXPERTS]
    full_b[0][...] = starts[EXPERTS : 2 * EXPERTS]
    halves[0][0][...] = starts[:EXPERTS]
    halves[1][0][...] = later[:EXPERTS]


def gather_kernel(map_ref, x_ref, other_hbm, diagonal_hbm, mate_hbm, *refs):
    slot_hbm, slot_refs = refs[:12], refs[12:24]
    maps, held, map_send, map_recv, far_send, far_recv, hop_send, hop_recv, near_send, near_recv, out_sems, slot_sems = refs[24:]
    me = lax.axis_index("ep")
    mate = me + 1 - 2 * lax.rem(me, 2)
    other = lax.rem(me + 2, 4)
    diagonal = lax.rem(mate + 2, 4)
    pieces = far_send.shape[0]
    size = x_ref.shape[0] // pieces

    def send(src, dst, send_sem, recv_sem, to):
        return pltpu.make_async_remote_copy(
            src_ref=src, dst_ref=dst, send_sem=send_sem, recv_sem=recv_sem,
            device_id={"ep": to}, device_id_type=pl.DeviceIdType.MESH,
        )

    barrier = pltpu.get_barrier_semaphore()
    for peer in (other, diagonal, mate):
        pl.semaphore_signal(barrier, inc=1, device_id={"ep": peer}, device_id_type=pl.DeviceIdType.MESH)
    pl.semaphore_wait(barrier, 3)

    map_copies = [send(map_ref, maps.at[i], map_send.at[i], map_recv.at[i], to) for i, to in enumerate((other, diagonal, mate))]
    for copy in map_copies:
        copy.start()
    part = [pl.ds(p * size, size) for p in range(pieces)]
    far = [send(x_ref.at[part[p], :], held.at[0, part[p], :], far_send.at[p], far_recv.at[p], other) for p in range(pieces)]
    for copy in far:
        copy.start()
    near = send(x_ref, held.at[2], near_send, near_recv, mate)
    near.start()
    for copy in map_copies:
        copy.wait_recv()
    find_slots((maps.at[0], maps.at[1], map_ref, maps.at[2]), slot_refs)
    slot_copies = [pltpu.make_async_copy(v, h, slot_sems.at[i]) for i, (v, h) in enumerate(zip(slot_refs, slot_hbm))]
    for copy in slot_copies:
        copy.start()
    near.wait()
    outs = [pltpu.make_async_copy(held.at[2], mate_hbm, out_sems.at[2 * pieces])]
    outs[0].start()
    hops = []
    for p in range(pieces):
        far[p].wait_recv()
        hops.append(send(held.at[0, part[p], :], held.at[1, part[p], :], hop_send.at[p], hop_recv.at[p], mate))
        hops[p].start()
        outs.append(pltpu.make_async_copy(held.at[0, part[p], :], other_hbm.at[part[p], :], out_sems.at[p]))
        outs[-1].start()
    for p in range(pieces):
        hops[p].wait_recv()
        outs.append(pltpu.make_async_copy(held.at[1, part[p], :], diagonal_hbm.at[part[p], :], out_sems.at[pieces + p]))
        outs[-1].start()
    for copy in map_copies + far + hops:
        copy.wait_send()
    for copy in outs + slot_copies:
        copy.wait()


def weight_copies(hbm, vmem, sems, e):
    return [pltpu.make_async_copy(h.at[e], v.at[e], sems.at[e, i]) for i, (h, v) in enumerate(zip(hbm, vmem))]


def forward_kernel(n, m, starts_ref, *refs):
    xs, (rows_ref, cols_ref, w1_hbm, w3_hbm, w2_hbm), ys = refs[:n], refs[n : n + 5], refs[n + 5 : n + m + 5]
    w1, w3, w2, u_all, o_all, h_ref, y_buf, w_sems, y_sems = refs[n + m + 5 :]
    blocks = rows_ref.shape[1] // TOKS
    width = w1.shape[2]
    slots = Slots(starts_ref, rows_ref, cols_ref, blocks)
    for e in range(EXPERTS):
        for copy in weight_copies((w1_hbm, w3_hbm, w2_hbm), (w1, w3, w2), w_sems, e):
            copy.start()

    def tokens_of(b):
        ref, toks = block_of(xs, b)
        return ref[toks, :]

    def gather_rows(e, carry):
        slots.compact(e, (tokens_of,), (u_all.at[e],))
        return carry

    lax.fori_loop(0, EXPERTS, gather_rows, 0)

    def expert(e, carry):
        for copy in weight_copies((w1_hbm, w3_hbm, w2_hbm), (w1, w3, w2), w_sems, e):
            copy.wait()

        def tile(k, inner):
            u = u_all[e, tile_rows(k), :]
            for c in range(0, width, COLS):
                cols = slice(c, c + COLS)
                a = mm(u, w1[e, :, cols])
                b = mm(u, w3[e, :, cols])
                h_ref[:, cols] = (a * jax.nn.sigmoid(a) * b).astype(BF)
            o_all[e, tile_rows(k), :] = mm(h_ref[...], w2[e]).astype(BF)
            return inner

        return lax.fori_loop(0, slots.tiles(e), tile, carry)

    lax.fori_loop(0, EXPERTS, expert, 0)
    for e in range(EXPERTS):
        slots.zero_after(e, o_all.at[e])
    each = ys[0].shape[0] // TOKS

    def send_home(i, carry):
        for j in range(each):
            b = i * each + j
            toks = slice(j * TOKS, (j + 1) * TOKS)
            y_buf[i, toks, :] = sum(slots.gate(e, b) * slots.spread(e, b, o_all.at[e]) for e in range(EXPERTS))
        for n, ref in enumerate(ys):
            pl.when(i == n)(lambda: pltpu.make_async_copy(y_buf.at[n], ref, y_sems.at[n]).start())
        return carry

    lax.fori_loop(0, len(ys), send_home, 0)
    for n, ref in enumerate(ys):
        pltpu.make_async_copy(y_buf.at[n], ref, y_sems.at[n]).wait()


def dx_kernel(n, starts_ref, *refs):
    xs, gs, (rows_ref, cols_ref, w1_hbm, w3_hbm, w2_hbm) = refs[:n], refs[n : n + 4], refs[n + 4 : n + 9]
    dxs, kept_hbm = refs[n + 9 : n + 13], refs[n + 13]
    w1, w3, w2, u_all, q_all, od_all, kept, dx_buf, w_sems, k_sems, dx_sems = refs[n + 14 :]
    tok = gs[0].shape[0]
    blocks = rows_ref.shape[1] // TOKS
    dim, width = w1.shape[1:]
    slots = Slots(starts_ref, rows_ref, cols_ref, blocks)
    for e in range(EXPERTS):
        for copy in weight_copies((w1_hbm, w3_hbm, w2_hbm), (w1, w3, w2), w_sems, e):
            copy.start()

    def tokens_of(b):
        ref, toks = block_of(xs, b)
        return ref[toks, :]

    def gather_rows(e, carry):
        def scaled_of(b):
            ref, toks = block_of(gs, b)
            return (slots.gate(e, b) * ref[toks, :].astype(F32)).astype(BF)

        slots.compact(e, (tokens_of, scaled_of), (u_all.at[e], q_all.at[e]))
        return carry

    lax.fori_loop(0, EXPERTS, gather_rows, 0)

    def copy_out(e, k, slot):
        return pltpu.make_async_copy(kept.at[slot], kept_hbm.at[e, tile_rows(k), :], k_sems.at[slot])

    def expert(e, carry):
        for copy in weight_copies((w1_hbm, w3_hbm, w2_hbm), (w1, w3, w2), w_sems, e):
            copy.wait()
        before = e * slots.tiles(0)

        def tile(k, inner):
            slot = lax.rem(before + k, 2)

            @pl.when(before + k >= 2)
            def _():
                copy_out(e, k, slot).wait()

            u = u_all[e, tile_rows(k), :]
            q = q_all[e, tile_rows(k), :]
            for c in range(0, width, COLS):
                cols = slice(c, c + COLS)
                a = mm(u, w1[e, :, cols])
                b = mm(u, w3[e, :, cols])
                dh = mm_nt(q, w2[e, cols, :])
                s = jax.nn.sigmoid(a)
                act = a * s
                kept[slot, :, c : c + COLS] = (act * b).astype(BF)
                kept[slot, :, width + c : width + c + COLS] = (dh * b * s * (1.0 + a * (1.0 - s))).astype(BF)
                kept[slot, :, 2 * width + c : 2 * width + c + COLS] = (dh * act).astype(BF)
            kept[slot, :, 3 * width : 3 * width + dim] = u
            kept[slot, :, 3 * width + dim :] = q
            od_all[e, tile_rows(k), :dim] = mm(kept[slot, :, :width], w2[e]).astype(BF)
            du = mm_nt(kept[slot, :, width : 2 * width], w1[e]) + mm_nt(kept[slot, :, 2 * width : 3 * width], w3[e])
            od_all[e, tile_rows(k), dim:] = du.astype(BF)
            copy_out(e, k, slot).start()
            return inner

        lax.fori_loop(0, slots.tiles(e), tile, 0)
        return carry

    lax.fori_loop(0, EXPERTS, expert, 0)
    for e in range(EXPERTS):
        slots.zero_after(e, od_all.at[e])
    copies = []
    each = tok // TOKS
    lane = lax.broadcasted_iota(jnp.int32, (TOKS, 8), 1).astype(F32)
    for i, ref in enumerate(dxs):

        for j in range(each):
            b = i * each + j
            toks = slice(j * TOKS, (j + 1) * TOKS)
            dy = gs[i][toks, :].astype(F32)
            dx = jnp.zeros((TOKS, dim), F32)
            dg = jnp.zeros((TOKS, 8), F32)
            for e in range(EXPERTS):
                od = slots.spread(e, b, od_all.at[e], ALIGN)
                dx += od[:, dim:]
                dg += jnp.where(lane == slots.choice(e, b), jnp.sum(dy * od[:, :dim], axis=1, keepdims=True), 0.0)
            dx_buf[i, toks, :] = dx
            dx_buf[i, tok : tok + 8, toks] = dg.T
        copies.append(pltpu.make_async_copy(dx_buf.at[i], ref, dx_sems.at[i]))
        copies[-1].start()
    for copy in copies:
        copy.wait()
    for slot in range(2):
        copy_out(0, 0, slot).wait()


def dw_kernel(starts_ref, kept_hbm, dw1_hbm, dw3_hbm, dw2_hbm, kept, dw1, dw3, dw2, k_sems, o_sems):
    dim, width = dw1.shape[1:]
    slots = Slots(starts_ref, None, None, kept_hbm.shape[1] // TOKS)

    def copy_in(e, k, slot):
        rows = pl.ds(pl.multiple_of(k * 2 * ROWS, 2 * ROWS), 2 * ROWS)
        return pltpu.make_async_copy(kept_hbm.at[e, rows, :], kept.at[slot], k_sems.at[slot])

    def copy_out(e, i):
        return pltpu.make_async_copy((dw1, dw3, dw2)[i].at[e], (dw1_hbm, dw3_hbm, dw2_hbm)[i].at[e], o_sems.at[e, i])

    first = (slots.tiles(1) > slots.tiles(0)).astype(jnp.int32)
    first_tiles = (slots.tiles(first) + 1) // 2
    count = first_tiles + (slots.tiles(1 - first) + 1) // 2

    def where(g):
        second = (g >= first_tiles).astype(jnp.int32)
        return jnp.where(second == 0, first, 1 - first), g - second * first_tiles

    copy_in(*where(0), 0).start()

    def tile(g, carry):
        slot = lax.rem(g, 2)
        e, k = where(g)
        copy_in(e, k, slot).wait()

        @pl.when(g + 1 < count)
        def _():
            copy_in(*where(g + 1), 1 - slot).start()

        @pl.when(2 * k + 1 == slots.tiles(e))
        def _():
            kept[slot, ROWS:, :] = jnp.zeros((ROWS, kept.shape[2]), BF)

        u = kept[slot, :, 3 * width : 3 * width + dim]
        q = kept[slot, :, 3 * width + dim :]
        fresh = k == 0
        last = (g == first_tiles - 1) | (g == count - 1)

        def put(ref, index, part):
            ref[index] = jnp.where(fresh, part, ref[index] + part)

        def leave(i):
            pl.when(last)(lambda: copy_out(e, i).start())

        for c in range(0, width, COLS):
            put(dw1, (e, slice(None), slice(c, c + COLS)), mm_tn(u, kept[slot, :, width + c : width + c + COLS]))
        leave(0)
        for c in range(0, width, COLS):
            put(dw3, (e, slice(None), slice(c, c + COLS)), mm_tn(u, kept[slot, :, 2 * width + c : 2 * width + c + COLS]))
        leave(1)
        for c in range(0, width, COLS):
            put(dw2, (e, slice(c, c + COLS), slice(None)), mm_tn(kept[slot, :, c : c + COLS], q))
        leave(2)
        return carry

    lax.fori_loop(0, count, tile, 0)
    for e in range(EXPERTS):
        for i in range(3):
            copy_out(e, i).wait()


IN_VMEM = pl.BlockSpec(memory_space=pltpu.VMEM)
IN_SMEM = pl.BlockSpec(memory_space=pltpu.SMEM)
IN_HBM = pl.BlockSpec(memory_space=pl.ANY)


def call(kernel, operands, in_specs, outs, out_specs, scratch, flops):
    return pl.pallas_call(
        kernel,
        in_specs=in_specs,
        out_specs=out_specs,
        out_shape=outs,
        scratch_shapes=scratch,
        compiler_params=pltpu.CompilerParams(vmem_limit_bytes=VMEM),
        cost_estimate=pl.CostEstimate(flops=flops, bytes_accessed=40_000_000, transcendentals=0),
    )(*operands)


def run_gather(own_map, x):
    tok, dim = x.shape
    tokens = 4 * tok
    pieces = 4
    outs = []
    for size in (tokens, tokens, tokens // 2, tokens // 2):
        outs.append(jax.ShapeDtypeStruct((EXPERTS, 128), jnp.int32))
        outs.append(jax.ShapeDtypeStruct((EXPERTS, size), F32))
        outs.append(jax.ShapeDtypeStruct((size, 8), F32))
    dma = pltpu.SemaphoreType.DMA
    out = pl.pallas_call(
        gather_kernel,
        in_specs=[IN_VMEM] * 2,
        out_specs=[IN_HBM] * 15,
        out_shape=[jax.ShapeDtypeStruct((tok, dim), BF)] * 3 + outs,
        scratch_shapes=[pltpu.VMEM(out.shape, out.dtype) for out in outs]
        + [pltpu.VMEM((3, *own_map.shape), F32), pltpu.VMEM((3, tok, dim), BF)]
        + [dma((3,)), dma((3,))] + [dma((pieces,))] * 4 + [dma, dma, dma((2 * pieces + 1,)), dma((12,))],
        compiler_params=pltpu.CompilerParams(collective_id=0, has_side_effects=True, vmem_limit_bytes=VMEM),
        cost_estimate=pl.CostEstimate(flops=10_000_000, bytes_accessed=4_000_000, transcendentals=0),
        name="gather_slots",
    )(own_map, x)
    maps = out[3:]
    return (out[0], out[1], x, out[2]), (maps[0:3], maps[3:6], maps[6:9], maps[9:12])


def weight_scratch(w1, w2):
    return [pltpu.VMEM(w1.shape, BF), pltpu.VMEM(w1.shape, BF), pltpu.VMEM(w2.shape, BF)]


def run_forward(tok, xs, maps, w1, w3, w2):
    dim = xs[0].shape[1]
    tokens = sum(x.shape[0] for x in xs)
    parts = tokens // tok
    width = w1.shape[2]
    most = tokens + TOKS + ALIGN + ROWS
    return call(
        functools.partial(forward_kernel, len(xs), parts), (maps[0], *xs, maps[1], maps[2], w1, w3, w2),
        [IN_SMEM] + [IN_VMEM] * (len(xs) + 2) + [IN_HBM] * 3,
        [jax.ShapeDtypeStruct((tok, dim), F32)] * parts,
        [IN_HBM] * parts,
        weight_scratch(w1, w2)
        + [pltpu.VMEM((EXPERTS, most, dim), BF)] * 2
        + [pltpu.VMEM((ROWS, width), BF), pltpu.VMEM((parts, tok, dim), F32)]
        + [pltpu.SemaphoreType.DMA((EXPERTS, 3)), pltpu.SemaphoreType.DMA((parts,))],
        2 * 3 * tokens * dim * width,
    )


def run_dx(xs, gs, maps, w1, w3, w2):
    tok, dim = gs[0].shape
    tokens = tok * len(gs)
    width = w1.shape[2]
    most = tokens + TOKS + ALIGN + ROWS
    kept = 3 * width + 2 * dim
    out = call(
        functools.partial(dx_kernel, len(xs)), (maps[0], *xs, *gs, maps[1], maps[2], w1, w3, w2),
        [IN_SMEM] + [IN_VMEM] * (len(xs) + 6) + [IN_HBM] * 3,
        [jax.ShapeDtypeStruct((tok + 8, dim), F32)] * 4 + [jax.ShapeDtypeStruct((EXPERTS, tokens, kept), BF)],
        [IN_HBM] * 5,
        weight_scratch(w1, w2)
        + [pltpu.VMEM((EXPERTS, most, dim), BF)] * 2
        + [pltpu.VMEM((EXPERTS, most, 2 * dim), BF), pltpu.VMEM((2, ROWS, kept), BF), pltpu.VMEM((4, tok + 8, dim), F32)]
        + [pltpu.SemaphoreType.DMA((EXPERTS, 3)), pltpu.SemaphoreType.DMA((2,)), pltpu.SemaphoreType.DMA((4,))],
        2 * 6 * tokens * dim * width,
    )
    return out[:4], out[4]


def run_dw(kept, maps, shape1, shape2):
    tokens = kept.shape[1]
    return call(
        dw_kernel, (maps[0], kept),
        [IN_SMEM, IN_HBM],
        [jax.ShapeDtypeStruct(shape1, F32), jax.ShapeDtypeStruct(shape1, F32), jax.ShapeDtypeStruct(shape2, F32)],
        [IN_HBM] * 3,
        [pltpu.VMEM((2, 2 * ROWS, kept.shape[2]), BF), pltpu.VMEM(shape1, F32), pltpu.VMEM(shape1, F32), pltpu.VMEM(shape2, F32)]
        + [pltpu.SemaphoreType.DMA((2,)), pltpu.SemaphoreType.DMA((EXPERTS, 3))],
        2 * 3 * tokens * shape1[1] * shape1[2],
    )


def solution(mesh):
    tok_spec = P(("dp", "ep"))
    w_spec = P("ep")
    across = [(0, 2), (2, 0), (1, 3), (3, 1)]
    beside = [(0, 1), (1, 0), (2, 3), (3, 2)]
    cross = [(0, 3), (3, 0), (1, 2), (2, 1)]

    def permute(v, pairs):
        return lax.ppermute(v, "ep", pairs)

    def gather(own):
        other = permute(own, across)
        return other, permute(other, beside), own, permute(own, beside)

    def gather_direct(own):
        return permute(own, across), permute(own, cross), own, permute(own, beside)

    def combine(parts):
        other, diagonal, own, mate = parts
        theirs = other + permute(diagonal, beside)
        return own + permute(mate, beside) + permute(theirs, across)

    def device_program(x_in, idx_a, idx_b, gate_a, gate_b, dy_out, w1_a, w3_a, w2_a, w1_b, w3_b, w2_b):
        tok, top_k = idx_a.shape
        own_map = jnp.concatenate([idx_a.astype(F32), idx_b.astype(F32), gate_a, gate_b], axis=1).T
        x_all, (maps_a, maps_b, maps_far, maps_near) = run_gather(own_map, x_in)

        def add(base, total):
            return (base.astype(F32) + total[:tok]).astype(BF)

        def dgate_of(total):
            return total[tok : tok + top_k].T

        dy_own, x_other = lax.optimization_barrier((dy_out, x_all[0]))
        x_all = (x_other, *x_all[1:])
        dy_all = gather(dy_own)
        other, diagonal = run_forward(tok, x_all[:2], maps_far, w1_a, w3_a, w2_a)
        own, mate = run_forward(tok, x_all[2:], maps_near, w1_a, w3_a, w2_a)
        diagonal = permute(diagonal, beside)
        mate = permute(mate, beside)
        half = tok // 2
        pieces = []
        for i in range(2):
            rows = slice(i * half, (i + 1) * half)
            theirs = permute(other[rows] + diagonal[rows], across)
            if pieces:
                theirs, _ = lax.optimization_barrier((theirs, pieces[0]))
            pieces.append((x_in[rows].astype(F32) + own[rows] + mate[rows] + theirs).astype(BF))
        gathered = [gather(piece) for piece in pieces]
        mid_all = [part for pair in zip(*gathered) for part in pair]
        x_mid = jnp.concatenate(pieces)
        x_again, mid_all[1] = lax.optimization_barrier((x_in, mid_all[1]))
        again_all = gather_direct(x_again)
        dx_parts, kept_b = run_dx(mid_all, dy_all, maps_b, w1_b, w3_b, w2_b)
        total = combine(dx_parts)
        dx_mid, dgate_b = add(dy_out, total), dgate_of(total)
        dmid_all = gather_direct(dx_mid)
        x_out = add(x_mid, combine(run_forward(tok, mid_all, maps_b, w1_b, w3_b, w2_b)))
        grads_b = run_dw(kept_b, maps_b, w1_b.shape, w2_b.shape)
        dx_parts, kept_a = run_dx(again_all, dmid_all, maps_a, w1_a, w3_a, w2_a)
        total = combine(dx_parts)
        dx_in, dgate_a = add(dx_mid, total), dgate_of(total)
        grads_a = run_dw(kept_a, maps_a, w1_a.shape, w2_a.shape)
        return (x_out, dx_in, *grads_a, *grads_b, dgate_a, dgate_b)


    return jax.shard_map(device_program, mesh=mesh, in_specs=(tok_spec,) * 6 + (w_spec,) * 6, out_specs=(tok_spec,) * 10, check_vma=False)
```

```python
import functools

import jax
import jax.numpy as jnp
from jax import lax
from jax.experimental import pallas as pl
from jax.experimental.pallas import tpu as pltpu
from jax.sharding import PartitionSpec as P


ROWS = 256
TOKS = 256
ALIGN = 16
COLS = 256
EXPERTS = 2
VMEM = 66_000_000

BF = jnp.bfloat16
F32 = jnp.float32


def mm(a, b):
    return lax.dot_general(a, b, (((1,), (0,)), ((), ())), preferred_element_type=F32)


def mm_nt(a, b):
    return lax.dot_general(a, b, (((1,), (1,)), ((), ())), preferred_element_type=F32)


def mm_tn(a, b):
    return lax.dot_general(a, b, (((0,), (0,)), ((), ())), preferred_element_type=F32)


def block_of(refs, b):
    per = refs[0].shape[0] // TOKS
    return refs[b // per], slice((b % per) * TOKS, (b % per + 1) * TOKS)


def tile_rows(k):
    return pl.ds(pl.multiple_of(k * ROWS, ROWS), ROWS)


class Slots:
    def __init__(self, starts_ref, rows_ref, cols_ref, blocks):
        self.starts_ref, self.rows_ref, self.cols_ref, self.blocks = starts_ref, rows_ref, cols_ref, blocks

    def tiles(self, e):
        return (self.starts_ref[e, self.blocks] + ROWS - 1) // ROWS

    def rows(self, e, b):
        return pl.ds(pl.multiple_of(self.starts_ref[e, b], ALIGN), TOKS)

    def base(self, e, b):
        return self.starts_ref[e, b].astype(F32)

    def col(self, b, i):
        rows = slice(b * TOKS, (b + 1) * TOKS) if isinstance(b, int) else pl.ds(pl.multiple_of(b * TOKS, TOKS), TOKS)
        return self.cols_ref[rows, i : i + 1]

    def gate(self, e, b):
        if isinstance(e, int):
            return self.col(b, EXPERTS + e)
        return jnp.where(e == 0, self.col(b, EXPERTS), self.col(b, EXPERTS + 1))

    def choice(self, e, b):
        return self.col(b, 2 * EXPERTS + e)

    def compact(self, e, makers, outs):
        line = lax.broadcasted_iota(jnp.int32, (TOKS, TOKS), 0).astype(F32)
        for b in range(self.blocks):
            slot = self.rows_ref[pl.ds(e, 1), b * TOKS : (b + 1) * TOKS] - self.base(e, b)
            hot = jnp.where(slot == line, 1.0, 0.0).astype(BF)
            for make, out in zip(makers, outs):
                out[self.rows(e, b), :] = mm(hot, make(b)).astype(BF)
        end = pl.multiple_of(self.starts_ref[e, self.blocks - 1] + TOKS, ALIGN)
        for out in outs:
            out[pl.ds(end, ROWS), :] = jnp.zeros((ROWS, out.shape[1]), BF)

    def spread(self, e, b, ref, more=0):
        line = lax.broadcasted_iota(jnp.int32, (TOKS, TOKS + more), 1).astype(F32)
        hot = jnp.where(self.col(b, e) - self.base(e, b) == line, 1.0, 0.0).astype(BF)
        rows = pl.ds(pl.multiple_of(self.starts_ref[e, b], ALIGN), TOKS + more)
        return mm(hot, ref[rows, :])

    def zero_after(self, e, ref):
        end = pl.multiple_of(self.tiles(e) * ROWS, ROWS)
        ref[pl.ds(end, TOKS + ALIGN), :] = jnp.zeros((TOKS + ALIGN, ref.shape[1]), BF)


def find_slots(tables, refs):
    full_a, full_b, halves = refs[0:3], refs[3:6], (refs[6:9], refs[9:12])
    tok = tables[0].shape[1]
    blocks = len(tables) * tok // TOKS
    half = blocks // 2
    first = (lax.axis_index("ep") * EXPERTS).astype(F32)
    line = lax.broadcasted_iota(jnp.int32, (8, TOKS), 0)
    target = first + (line % EXPERTS).astype(F32)
    lane = lax.broadcasted_iota(jnp.int32, (8, 128), 1)
    upto = (lax.broadcasted_iota(jnp.int32, (TOKS, TOKS), 0) <= lax.broadcasted_iota(jnp.int32, (TOKS, TOKS), 1)).astype(F32).astype(BF)
    seen = jnp.zeros((8, 1), F32)
    before = jnp.zeros((8, 1), F32)
    starts = jnp.zeros((8, 128), F32)
    later = jnp.zeros((8, 128), F32)
    for b in range(blocks):
        at = b * TOKS
        table = tables[at // tok][:, at % tok : at % tok + TOKS]
        if b == half:
            before = seen

        def both(i, other):
            return jnp.where(line < EXPERTS, table[i : i + 1], jnp.where(line < 2 * EXPERTS, table[i + 2 : i + 3], other))

        hit0 = both(0, -1.0) == target
        hit1 = both(1, -1.0) == target
        mask = jnp.where(hit0 | hit1, 1.0, 0.0)
        count = mm(mask.astype(BF), upto)
        slot = jnp.where(mask > 0.0, seen + count - 1.0, -1.0)
        part_slot = jnp.where(mask > 0.0, seen - before + count - 1.0, -1.0)
        gate = jnp.where(hit0, both(4, 0.0), 0.0) + jnp.where(hit1, both(5, 0.0), 0.0)
        choice = jnp.where(hit1, 1.0, 0.0)
        starts = jnp.where(lane == b, seen, starts)
        if b >= half:
            later = jnp.where(lane == b - half, seen - before, later)

        def put(outs, layer, here, slots):
            part = slice(layer * EXPERTS, (layer + 1) * EXPERTS)
            outs[1][:, here : here + TOKS] = slots[part]
            stack = jnp.concatenate([slots[part], gate[part], choice[part], choice[part]], axis=0)
            outs[2][here : here + TOKS, :] = stack.T

        put(full_a, 0, at, slot)
        put(full_b, 1, at, slot)
        put(halves[b // half], 0, at % (half * TOKS), part_slot)
        seen = seen + jnp.floor((count[:, TOKS - 1 :] + (ALIGN - 1.0)) / ALIGN) * ALIGN
    starts = jnp.where(lane == blocks, seen, starts).astype(jnp.int32)
    later = jnp.where(lane == half, seen - before, later).astype(jnp.int32)
    full_a[0][...] = starts[:EXPERTS]
    full_b[0][...] = starts[EXPERTS : 2 * EXPERTS]
    halves[0][0][...] = starts[:EXPERTS]
    halves[1][0][...] = later[:EXPERTS]


def gather_kernel(map_ref, x_ref, other_hbm, diagonal_hbm, mate_hbm, *refs):
    slot_hbm, slot_refs = refs[:12], refs[12:24]
    maps, held, map_send, map_recv, far_send, far_recv, hop_send, hop_recv, near_send, near_recv, out_sems, slot_sems = refs[24:]
    me = lax.axis_index("ep")
    mate = me + 1 - 2 * lax.rem(me, 2)
    other = lax.rem(me + 2, 4)
    diagonal = lax.rem(mate + 2, 4)
    pieces = far_send.shape[0]
    size = x_ref.shape[0] // pieces

    def send(src, dst, send_sem, recv_sem, to):
        return pltpu.make_async_remote_copy(
            src_ref=src, dst_ref=dst, send_sem=send_sem, recv_sem=recv_sem,
            device_id={"ep": to}, device_id_type=pl.DeviceIdType.MESH,
        )

    barrier = pltpu.get_barrier_semaphore()
    for peer in (other, diagonal, mate):
        pl.semaphore_signal(barrier, inc=1, device_id={"ep": peer}, device_id_type=pl.DeviceIdType.MESH)
    pl.semaphore_wait(barrier, 3)

    map_copies = [send(map_ref, maps.at[i], map_send.at[i], map_recv.at[i], to) for i, to in enumerate((other, diagonal, mate))]
    for copy in map_copies:
        copy.start()
    part = [pl.ds(p * size, size) for p in range(pieces)]
    far = [send(x_ref.at[part[p], :], held.at[0, part[p], :], far_send.at[p], far_recv.at[p], other) for p in range(pieces)]
    for copy in far:
        copy.start()
    near = send(x_ref, held.at[2], near_send, near_recv, mate)
    near.start()
    for copy in map_copies:
        copy.wait_recv()
    find_slots((maps.at[0], maps.at[1], map_ref, maps.at[2]), slot_refs)
    slot_copies = [pltpu.make_async_copy(v, h, slot_sems.at[i]) for i, (v, h) in enumerate(zip(slot_refs, slot_hbm))]
    for copy in slot_copies:
        copy.start()
    near.wait()
    outs = [pltpu.make_async_copy(held.at[2], mate_hbm, out_sems.at[2 * pieces])]
    outs[0].start()
    hops = []
    for p in range(pieces):
        far[p].wait_recv()
        hops.append(send(held.at[0, part[p], :], held.at[1, part[p], :], hop_send.at[p], hop_recv.at[p], mate))
        hops[p].start()
        outs.append(pltpu.make_async_copy(held.at[0, part[p], :], other_hbm.at[part[p], :], out_sems.at[p]))
        outs[-1].start()
    for p in range(pieces):
        hops[p].wait_recv()
        outs.append(pltpu.make_async_copy(held.at[1, part[p], :], diagonal_hbm.at[part[p], :], out_sems.at[pieces + p]))
        outs[-1].start()
    for copy in map_copies + far + hops:
        copy.wait_send()
    for copy in outs + slot_copies:
        copy.wait()


def weight_copies(hbm, vmem, sems, e):
    return [pltpu.make_async_copy(h.at[e], v.at[e], sems.at[e, i]) for i, (h, v) in enumerate(zip(hbm, vmem))]


def forward_kernel(n, m, starts_ref, *refs):
    xs, (rows_ref, cols_ref, w1_hbm, w3_hbm, w2_hbm), ys = refs[:n], refs[n : n + 5], refs[n + 5 : n + m + 5]
    w1, w3, w2, u_all, o_all, h_ref, y_buf, w_sems, y_sems = refs[n + m + 5 :]
    blocks = rows_ref.shape[1] // TOKS
    width = w1.shape[2]
    slots = Slots(starts_ref, rows_ref, cols_ref, blocks)
    for e in range(EXPERTS):
        for copy in weight_copies((w1_hbm, w3_hbm, w2_hbm), (w1, w3, w2), w_sems, e):
            copy.start()

    def tokens_of(b):
        ref, toks = block_of(xs, b)
        return ref[toks, :]

    def gather_rows(e, carry):
        slots.compact(e, (tokens_of,), (u_all.at[e],))
        return carry

    lax.fori_loop(0, EXPERTS, gather_rows, 0)

    def expert(e, carry):
        for copy in weight_copies((w1_hbm, w3_hbm, w2_hbm), (w1, w3, w2), w_sems, e):
            copy.wait()

        def tile(k, inner):
            u = u_all[e, tile_rows(k), :]
            for c in range(0, width, COLS):
                cols = slice(c, c + COLS)
                a = mm(u, w1[e, :, cols])
                b = mm(u, w3[e, :, cols])
                h_ref[:, cols] = (a * jax.nn.sigmoid(a) * b).astype(BF)
            o_all[e, tile_rows(k), :] = mm(h_ref[...], w2[e]).astype(BF)
            return inner

        return lax.fori_loop(0, slots.tiles(e), tile, carry)

    lax.fori_loop(0, EXPERTS, expert, 0)
    for e in range(EXPERTS):
        slots.zero_after(e, o_all.at[e])
    each = ys[0].shape[0] // TOKS

    def send_home(i, carry):
        for j in range(each):
            b = i * each + j
            toks = slice(j * TOKS, (j + 1) * TOKS)
            y_buf[i, toks, :] = sum(slots.gate(e, b) * slots.spread(e, b, o_all.at[e]) for e in range(EXPERTS))
        for n, ref in enumerate(ys):
            pl.when(i == n)(lambda: pltpu.make_async_copy(y_buf.at[n], ref, y_sems.at[n]).start())
        return carry

    lax.fori_loop(0, len(ys), send_home, 0)
    for n, ref in enumerate(ys):
        pltpu.make_async_copy(y_buf.at[n], ref, y_sems.at[n]).wait()


def dx_kernel(n, starts_ref, *refs):
    xs, gs, (rows_ref, cols_ref, w1_hbm, w3_hbm, w2_hbm) = refs[:n], refs[n : n + 4], refs[n + 4 : n + 9]
    dxs, kept_hbm = refs[n + 9 : n + 13], refs[n + 13]
    w1, w3, w2, u_all, q_all, od_all, kept, dx_buf, w_sems, k_sems, dx_sems = refs[n + 14 :]
    tok = gs[0].shape[0]
    blocks = rows_ref.shape[1] // TOKS
    dim, width = w1.shape[1:]
    slots = Slots(starts_ref, rows_ref, cols_ref, blocks)
    for e in range(EXPERTS):
        for copy in weight_copies((w1_hbm, w3_hbm, w2_hbm), (w1, w3, w2), w_sems, e):
            copy.start()

    def tokens_of(b):
        ref, toks = block_of(xs, b)
        return ref[toks, :]

    def gather_rows(e, carry):
        def scaled_of(b):
            ref, toks = block_of(gs, b)
            return (slots.gate(e, b) * ref[toks, :].astype(F32)).astype(BF)

        slots.compact(e, (tokens_of, scaled_of), (u_all.at[e], q_all.at[e]))
        return carry

    lax.fori_loop(0, EXPERTS, gather_rows, 0)

    def copy_out(e, k, slot):
        return pltpu.make_async_copy(kept.at[slot], kept_hbm.at[e, tile_rows(k), :], k_sems.at[slot])

    def expert(e, carry):
        for copy in weight_copies((w1_hbm, w3_hbm, w2_hbm), (w1, w3, w2), w_sems, e):
            copy.wait()
        before = e * slots.tiles(0)

        def tile(k, inner):
            slot = lax.rem(before + k, 2)

            @pl.when(before + k >= 2)
            def _():
                copy_out(e, k, slot).wait()

            u = u_all[e, tile_rows(k), :]
            q = q_all[e, tile_rows(k), :]
            for c in range(0, width, COLS):
                cols = slice(c, c + COLS)
                a = mm(u, w1[e, :, cols])
                b = mm(u, w3[e, :, cols])
                dh = mm_nt(q, w2[e, cols, :])
                s = jax.nn.sigmoid(a)
                act = a * s
                kept[slot, :, c : c + COLS] = (act * b).astype(BF)
                kept[slot, :, width + c : width + c + COLS] = (dh * b * s * (1.0 + a * (1.0 - s))).astype(BF)
                kept[slot, :, 2 * width + c : 2 * width + c + COLS] = (dh * act).astype(BF)
            kept[slot, :, 3 * width : 3 * width + dim] = u
            kept[slot, :, 3 * width + dim :] = q
            od_all[e, tile_rows(k), :dim] = mm(kept[slot, :, :width], w2[e]).astype(BF)
            du = mm_nt(kept[slot, :, width : 2 * width], w1[e]) + mm_nt(kept[slot, :, 2 * width : 3 * width], w3[e])
            od_all[e, tile_rows(k), dim:] = du.astype(BF)
            copy_out(e, k, slot).start()
            return inner

        lax.fori_loop(0, slots.tiles(e), tile, 0)
        return carry

    lax.fori_loop(0, EXPERTS, expert, 0)
    for e in range(EXPERTS):
        slots.zero_after(e, od_all.at[e])
    copies = []
    each = tok // TOKS
    lane = lax.broadcasted_iota(jnp.int32, (TOKS, 8), 1).astype(F32)
    for i, ref in enumerate(dxs):

        for j in range(each):
            b = i * each + j
            toks = slice(j * TOKS, (j + 1) * TOKS)
            dy = gs[i][toks, :].astype(F32)
            dx = jnp.zeros((TOKS, dim), F32)
            dg = jnp.zeros((TOKS, 8), F32)
            for e in range(EXPERTS):
                od = slots.spread(e, b, od_all.at[e], ALIGN)
                dx += od[:, dim:]
                dg += jnp.where(lane == slots.choice(e, b), jnp.sum(dy * od[:, :dim], axis=1, keepdims=True), 0.0)
            dx_buf[i, toks, :] = dx
            dx_buf[i, tok : tok + 8, toks] = dg.T
        copies.append(pltpu.make_async_copy(dx_buf.at[i], ref, dx_sems.at[i]))
        copies[-1].start()
    for copy in copies:
        copy.wait()
    for slot in range(2):
        copy_out(0, 0, slot).wait()


def dw_kernel(starts_ref, kept_hbm, dw1_hbm, dw3_hbm, dw2_hbm, kept, dw1, dw3, dw2, k_sems, o_sems):
    dim, width = dw1.shape[1:]
    slots = Slots(starts_ref, None, None, kept_hbm.shape[1] // TOKS)

    def copy_in(e, k, slot):
        rows = pl.ds(pl.multiple_of(k * 2 * ROWS, 2 * ROWS), 2 * ROWS)
        return pltpu.make_async_copy(kept_hbm.at[e, rows, :], kept.at[slot], k_sems.at[slot])

    def copy_out(e, i):
        return pltpu.make_async_copy((dw1, dw3, dw2)[i].at[e], (dw1_hbm, dw3_hbm, dw2_hbm)[i].at[e], o_sems.at[e, i])

    first = (slots.tiles(1) > slots.tiles(0)).astype(jnp.int32)
    first_tiles = (slots.tiles(first) + 1) // 2
    count = first_tiles + (slots.tiles(1 - first) + 1) // 2

    def where(g):
        second = (g >= first_tiles).astype(jnp.int32)
        return jnp.where(second == 0, first, 1 - first), g - second * first_tiles

    copy_in(*where(0), 0).start()

    def tile(g, carry):
        slot = lax.rem(g, 2)
        e, k = where(g)
        copy_in(e, k, slot).wait()

        @pl.when(g + 1 < count)
        def _():
            copy_in(*where(g + 1), 1 - slot).start()

        @pl.when(2 * k + 1 == slots.tiles(e))
        def _():
            kept[slot, ROWS:, :] = jnp.zeros((ROWS, kept.shape[2]), BF)

        u = kept[slot, :, 3 * width : 3 * width + dim]
        q = kept[slot, :, 3 * width + dim :]
        fresh = k == 0
        last = (g == first_tiles - 1) | (g == count - 1)

        def put(ref, index, part):
            ref[index] = jnp.where(fresh, part, ref[index] + part)

        def leave(i):
            pl.when(last)(lambda: copy_out(e, i).start())

        for c in range(0, width, COLS):
            put(dw1, (e, slice(None), slice(c, c + COLS)), mm_tn(u, kept[slot, :, width + c : width + c + COLS]))
        leave(0)
        for c in range(0, width, COLS):
            put(dw3, (e, slice(None), slice(c, c + COLS)), mm_tn(u, kept[slot, :, 2 * width + c : 2 * width + c + COLS]))
        leave(1)
        for c in range(0, width, COLS):
            put(dw2, (e, slice(c, c + COLS), slice(None)), mm_tn(kept[slot, :, c : c + COLS], q))
        leave(2)
        return carry

    lax.fori_loop(0, count, tile, 0)
    for e in range(EXPERTS):
        for i in range(3):
            copy_out(e, i).wait()


IN_VMEM = pl.BlockSpec(memory_space=pltpu.VMEM)
IN_SMEM = pl.BlockSpec(memory_space=pltpu.SMEM)
IN_HBM = pl.BlockSpec(memory_space=pl.ANY)


def call(kernel, operands, in_specs, outs, out_specs, scratch, flops):
    return pl.pallas_call(
        kernel,
        in_specs=in_specs,
        out_specs=out_specs,
        out_shape=outs,
        scratch_shapes=scratch,
        compiler_params=pltpu.CompilerParams(vmem_limit_bytes=VMEM),
        cost_estimate=pl.CostEstimate(flops=flops, bytes_accessed=40_000_000, transcendentals=0),
    )(*operands)


def run_gather(own_map, x):
    tok, dim = x.shape
    tokens = 4 * tok
    pieces = 8
    outs = []
    for size in (tokens, tokens, tokens // 2, tokens // 2):
        outs.append(jax.ShapeDtypeStruct((EXPERTS, 128), jnp.int32))
        outs.append(jax.ShapeDtypeStruct((EXPERTS, size), F32))
        outs.append(jax.ShapeDtypeStruct((size, 8), F32))
    dma = pltpu.SemaphoreType.DMA
    out = pl.pallas_call(
        gather_kernel,
        in_specs=[IN_VMEM] * 2,
        out_specs=[IN_HBM] * 15,
        out_shape=[jax.ShapeDtypeStruct((tok, dim), BF)] * 3 + outs,
        scratch_shapes=[pltpu.VMEM(out.shape, out.dtype) for out in outs]
        + [pltpu.VMEM((3, *own_map.shape), F32), pltpu.VMEM((3, tok, dim), BF)]
        + [dma((3,)), dma((3,))] + [dma((pieces,))] * 4 + [dma, dma, dma((2 * pieces + 1,)), dma((12,))],
        compiler_params=pltpu.CompilerParams(collective_id=0, has_side_effects=True, vmem_limit_bytes=VMEM),
        cost_estimate=pl.CostEstimate(flops=10_000_000, bytes_accessed=4_000_000, transcendentals=0),
        name="gather_slots",
    )(own_map, x)
    maps = out[3:]
    return (out[0], out[1], x, out[2]), (maps[0:3], maps[3:6], maps[6:9], maps[9:12])


def weight_scratch(w1, w2):
    return [pltpu.VMEM(w1.shape, BF), pltpu.VMEM(w1.shape, BF), pltpu.VMEM(w2.shape, BF)]


def run_forward(tok, xs, maps, w1, w3, w2):
    dim = xs[0].shape[1]
    tokens = sum(x.shape[0] for x in xs)
    parts = tokens // tok
    width = w1.shape[2]
    most = tokens + TOKS + ALIGN + ROWS
    return call(
        functools.partial(forward_kernel, len(xs), parts), (maps[0], *xs, maps[1], maps[2], w1, w3, w2),
        [IN_SMEM] + [IN_VMEM] * (len(xs) + 2) + [IN_HBM] * 3,
        [jax.ShapeDtypeStruct((tok, dim), F32)] * parts,
        [IN_HBM] * parts,
        weight_scratch(w1, w2)
        + [pltpu.VMEM((EXPERTS, most, dim), BF)] * 2
        + [pltpu.VMEM((ROWS, width), BF), pltpu.VMEM((parts, tok, dim), F32)]
        + [pltpu.SemaphoreType.DMA((EXPERTS, 3)), pltpu.SemaphoreType.DMA((parts,))],
        2 * 3 * tokens * dim * width,
    )


def run_dx(xs, gs, maps, w1, w3, w2):
    tok, dim = gs[0].shape
    tokens = tok * len(gs)
    width = w1.shape[2]
    most = tokens + TOKS + ALIGN + ROWS
    kept = 3 * width + 2 * dim
    out = call(
        functools.partial(dx_kernel, len(xs)), (maps[0], *xs, *gs, maps[1], maps[2], w1, w3, w2),
        [IN_SMEM] + [IN_VMEM] * (len(xs) + 6) + [IN_HBM] * 3,
        [jax.ShapeDtypeStruct((tok + 8, dim), F32)] * 4 + [jax.ShapeDtypeStruct((EXPERTS, tokens, kept), BF)],
        [IN_HBM] * 5,
        weight_scratch(w1, w2)
        + [pltpu.VMEM((EXPERTS, most, dim), BF)] * 2
        + [pltpu.VMEM((EXPERTS, most, 2 * dim), BF), pltpu.VMEM((2, ROWS, kept), BF), pltpu.VMEM((4, tok + 8, dim), F32)]
        + [pltpu.SemaphoreType.DMA((EXPERTS, 3)), pltpu.SemaphoreType.DMA((2,)), pltpu.SemaphoreType.DMA((4,))],
        2 * 6 * tokens * dim * width,
    )
    return out[:4], out[4]


def run_dw(kept, maps, shape1, shape2):
    tokens = kept.shape[1]
    return call(
        dw_kernel, (maps[0], kept),
        [IN_SMEM, IN_HBM],
        [jax.ShapeDtypeStruct(shape1, F32), jax.ShapeDtypeStruct(shape1, F32), jax.ShapeDtypeStruct(shape2, F32)],
        [IN_HBM] * 3,
        [pltpu.VMEM((2, 2 * ROWS, kept.shape[2]), BF), pltpu.VMEM(shape1, F32), pltpu.VMEM(shape1, F32), pltpu.VMEM(shape2, F32)]
        + [pltpu.SemaphoreType.DMA((2,)), pltpu.SemaphoreType.DMA((EXPERTS, 3))],
        2 * 3 * tokens * shape1[1] * shape1[2],
    )


def solution(mesh):
    tok_spec = P(("dp", "ep"))
    w_spec = P("ep")
    across = [(0, 2), (2, 0), (1, 3), (3, 1)]
    beside = [(0, 1), (1, 0), (2, 3), (3, 2)]
    cross = [(0, 3), (3, 0), (1, 2), (2, 1)]

    def permute(v, pairs):
        return lax.ppermute(v, "ep", pairs)

    def gather(own):
        other = permute(own, across)
        return other, permute(other, beside), own, permute(own, beside)

    def gather_direct(own):
        return permute(own, across), permute(own, cross), own, permute(own, beside)

    def combine(parts):
        other, diagonal, own, mate = parts
        theirs = other + permute(diagonal, beside)
        return own + permute(mate, beside) + permute(theirs, across)

    def device_program(x_in, idx_a, idx_b, gate_a, gate_b, dy_out, w1_a, w3_a, w2_a, w1_b, w3_b, w2_b):
        tok, top_k = idx_a.shape
        ids = jnp.concatenate([idx_a.T, idx_b.T]).astype(F32)
        own_map = jnp.concatenate([ids, gate_a.T, gate_b.T])
        x_all, (maps_a, maps_b, maps_far, maps_near) = run_gather(own_map, x_in)

        def add(base, total):
            return (base.astype(F32) + total[:tok]).astype(BF)

        def dgate_of(total):
            return total[tok : tok + top_k].T

        dy_own, x_other = lax.optimization_barrier((dy_out, x_all[0]))
        x_all = (x_other, *x_all[1:])
        dy_all = gather(dy_own)
        other, diagonal = run_forward(tok, x_all[:2], maps_far, w1_a, w3_a, w2_a)
        own, mate = run_forward(tok, x_all[2:], maps_near, w1_a, w3_a, w2_a)
        diagonal = permute(diagonal, beside)
        mate = permute(mate, beside)
        half = tok // 2
        pieces = []
        for i in range(2):
            rows = slice(i * half, (i + 1) * half)
            theirs = permute(other[rows] + diagonal[rows], across)
            if pieces:
                theirs, _ = lax.optimization_barrier((theirs, pieces[0]))
            pieces.append((x_in[rows].astype(F32) + own[rows] + mate[rows] + theirs).astype(BF))
        gathered = [gather(piece) for piece in pieces]
        mid_all = [part for pair in zip(*gathered) for part in pair]
        x_mid = jnp.concatenate(pieces)
        x_again, mid_all[1] = lax.optimization_barrier((x_in, mid_all[1]))
        again_all = gather_direct(x_again)
        dx_parts, kept_b = run_dx(mid_all, dy_all, maps_b, w1_b, w3_b, w2_b)
        total = combine(dx_parts)
        dx_mid, dgate_b = add(dy_out, total), dgate_of(total)
        dmid_all = gather_direct(dx_mid)
        x_out = add(x_mid, combine(run_forward(tok, mid_all, maps_b, w1_b, w3_b, w2_b)))
        grads_b = run_dw(kept_b, maps_b, w1_b.shape, w2_b.shape)
        dx_parts, kept_a = run_dx(again_all, dmid_all, maps_a, w1_a, w3_a, w2_a)
        total = combine(dx_parts)
        dx_in, dgate_a = add(dx_mid, total), dgate_of(total)
        grads_a = run_dw(kept_a, maps_a, w1_a.shape, w2_a.shape)
        return (x_out, dx_in, *grads_a, *grads_b, dgate_a, dgate_b)


    return jax.shard_map(device_program, mesh=mesh, in_specs=(tok_spec,) * 6 + (w_spec,) * 6, out_specs=(tok_spec,) * 10, check_vma=False)
```
